128 devices in a mesh: beta: 64 (over z, y, x), grp: 2 (over core).
Axes of the slice: x: 4, y: 4, z: 4, core: 2. Of those that a mesh axis runs over, the one named last changes fastest.
Arguments:
- samples: float32 [128, 8, 128, 128], P('beta', 'grp'), parts along dimension 1, may hold values from -6 to 6
Outputs:
- coeffs: float32 [128, 2, 8, 64, 64], P('beta', None, 'grp'), parts along dimension 2
- power: float32 [8, 64], P('grp'), parts along dimension 0
The draws below stay inside these ranges and needn't reach their ends.
There are 2 independent parts, one for each index of `grp`. The reference program is written for one: setup_inputs(seed, part) draws one part's arguments, and reference() takes and returns one part's arrays. A program takes and returns all parts, laid end to end along the dimension named above; each array names one. Nothing has to cross between parts.
All inputs are finite; a program needn't handle non-finite values.
Results may differ from the reference program's by a relative error of at most 0.0003.
Values sent between devices are 32-bit elements; how exact they have to be, the bound alone decides.
A program may use at most 64 MiB of HBM per device.

```python
import jax
import jax.numpy as jnp
from jax import lax

F = 4
GRID = 128


def shard_levels(key, dims, pieces, smallest, top_value):
    factor_of, own = 1.0, jax.random.fold_in(key, 6)
    for position, parts in pieces:
        draws = jnp.exp(jax.random.uniform(jax.random.fold_in(own, position), (parts,), jnp.float32, smallest / len(pieces), top_value / len(pieces)))
        factor_of = factor_of * jnp.repeat(draws, dims[position] // parts).reshape([-1 if axis == position else 1 for axis in range(len(dims))])
    return factor_of


def bell_draw(own_key, dims, scale, reach, shards=(), kind=jnp.bfloat16):
    result = jax.random.normal(own_key, dims, jnp.float32) * scale
    if len(shards) > 0:
        result = shard_levels(own_key, dims, shards, -0.22, 0.18) * result
    return jnp.clip(result, min=-reach, max=reach).astype(kind)


def setup_inputs(seed: int = 0, part: int = 0) -> dict:
    key_of = jax.random.split(jax.random.key(seed), 2)
    own_keys = jax.random.split(jax.random.fold_in(key_of[1], part), 2)
    return {
        "samples": bell_draw(own_keys[0], (GRID, F, GRID, GRID), 1.0, 6.0, ((0, 64),), jnp.float32),
    }


HIGHEST = lax.Precision.HIGHEST

def beta_angles(spread):
    grid_size = 2 * spread
    return (2.0 * jnp.arange(grid_size, dtype=jnp.float32) + 1.0) * (jnp.pi / (4.0 * spread))

def quadrature(spread):
    angles = beta_angles(spread)
    odd_terms = 2.0 * jnp.arange(spread, dtype=jnp.float32) + 1.0
    series = lax.optimization_barrier(jnp.sum(jnp.sin(angles[:, None] * odd_terms[None, :]) / odd_terms[None, :], axis=1))
    return 2.0 / spread * jnp.sin(angles) * series

def gamma_table(spread):
    grid_size = 2 * spread
    positions = jnp.arange(grid_size, dtype=jnp.int32)
    orders = jnp.arange(spread, dtype=jnp.int32)
    phase_index = positions[:, None] * orders[None, :] % grid_size
    angles = phase_index.astype(jnp.float32) * (2.0 * jnp.pi / grid_size)
    return jnp.concatenate([jnp.cos(angles), -jnp.sin(angles)], axis=1)

def alpha_table(spread, row_index):
    grid_size = 2 * spread
    positions = jnp.arange(grid_size, dtype=jnp.int32)
    phase_index = row_index[:, None] * positions[None, :] % grid_size
    angles = phase_index.astype(jnp.float32) * (2.0 * jnp.pi / grid_size)
    cosine = jnp.cos(angles) / grid_size
    sine_part = jnp.sin(angles) / grid_size
    real_rows = jnp.stack([cosine, sine_part], axis=1)
    imag_rows = jnp.stack([-sine_part, cosine], axis=1)
    return jnp.stack([real_rows, imag_rows], axis=0)

def log_factorial(value, float_type):
    return lax.lgamma((value + 1).astype(float_type))

def wigner_start(alpha_order, gamma_order, log_cosine, log_sine):
    float_type = log_cosine.dtype
    lowest = jnp.maximum(jnp.abs(alpha_order), gamma_order)
    shift_low = jnp.maximum(0, gamma_order - alpha_order)
    magnitude = 0.5 * (log_factorial(lowest + alpha_order, float_type) + log_factorial(lowest - alpha_order, float_type) + log_factorial(lowest + gamma_order, float_type) + log_factorial(lowest - gamma_order, float_type))
    magnitude = magnitude - log_factorial(lowest + gamma_order - shift_low, float_type) - log_factorial(shift_low, float_type)
    magnitude = magnitude - log_factorial(alpha_order - gamma_order + shift_low, float_type)
    magnitude = magnitude - log_factorial(lowest - alpha_order - shift_low, float_type)
    cos_power = (2 * lowest + gamma_order - alpha_order - 2 * shift_low).astype(float_type)
    sin_power = (alpha_order - gamma_order + 2 * shift_low).astype(float_type)
    parity = (alpha_order - gamma_order + shift_low) % 2
    sign_factor = (1 - 2 * parity).astype(float_type)
    return sign_factor * jnp.exp(magnitude + cos_power * log_cosine + sin_power * log_sine)

def advance(degree, carried, alpha_order, gamma_order, cos_angles, start_value, lowest):
    former, current = carried
    float_type = current.dtype
    previous = (degree - 1).astype(float_type)
    alpha_float = alpha_order.astype(float_type)
    gamma_float = gamma_order.astype(float_type)
    cross_ratio = alpha_float * gamma_float / jnp.maximum(previous * (previous + 1.0), 1.0)
    upper_term = ((previous + 1.0) * (previous + 1.0) - alpha_float * alpha_float) * ((previous + 1.0) * (previous + 1.0) - gamma_float * gamma_float)
    lower_term = (previous * previous - alpha_float * alpha_float) * (previous * previous - gamma_float * gamma_float)
    root_upper = jnp.sqrt(jnp.maximum(upper_term, 1.0))
    forward = (previous + 1.0) * (2.0 * previous + 1.0) / root_upper
    backward = (previous + 1.0) * jnp.sqrt(jnp.maximum(lower_term, 0.0)) / (jnp.maximum(previous, 1.0) * root_upper)
    recurred = forward * (cos_angles - cross_ratio) * current - backward * former
    renewed = jnp.where(degree == lowest, start_value, recurred)
    return (current, renewed)

def degree_group(row_index, weighted, spread):
    grid_size = 2 * spread
    alpha_order = jnp.where(row_index < spread, row_index, row_index - grid_size)[:, None, None]
    gamma_order = jnp.arange(spread, dtype=jnp.int32)[None, None, :]
    angles = beta_angles(spread)
    cos_angles = jnp.cos(angles)[None, :, None]
    log_cosine = jnp.log(jnp.cos(0.5 * angles))[None, :, None]
    log_sine = jnp.log(jnp.sin(0.5 * angles))[None, :, None]
    lowest = jnp.maximum(jnp.abs(alpha_order), gamma_order)
    start_value = wigner_start(alpha_order, gamma_order, log_cosine, log_sine)
    empty_state = jnp.zeros((row_index.shape[0], grid_size, spread), jnp.float32)

    def level_step(carried, degree):
        carried = advance(degree, carried, alpha_order, gamma_order, cos_angles, start_value, lowest)
        contribution = jnp.einsum('gkq,kgcq->gcq', carried[1], weighted, precision=HIGHEST)
        return (carried, contribution)
    _, stacked = lax.scan(level_step, (empty_state, empty_state), jnp.arange(spread, dtype=jnp.int32))
    degree_scale = 8.0 * jnp.sqrt(2.0 * jnp.arange(spread, dtype=jnp.float32) + 1.0)
    return jnp.transpose(stacked, (1, 2, 0, 3)) * degree_scale[None, None, :, None]

def degree_energy(coeffs, spread):
    multiplicity = jnp.where(jnp.arange(spread) == 0, 1.0, 2.0).astype(jnp.float32)
    energy_sum = lax.optimization_barrier(jnp.sum(coeffs * coeffs * multiplicity, axis=(0, 1, 4)))
    degrees = 2.0 * jnp.arange(spread, dtype=jnp.float32) + 1.0
    return energy_sum / (degrees * degrees)[None, :]

def reference(samples):
    grid_size = samples.shape[2]
    spread = grid_size // 2
    functions = samples.shape[1]
    channels = 2 * functions
    halfway = jnp.einsum('kfag,gx->kfax', samples, gamma_table(spread), precision=HIGHEST)
    halfway = halfway.reshape(grid_size, functions, grid_size, 2, spread)
    row_index = jnp.arange(grid_size, dtype=jnp.int32)
    spectrum = jnp.einsum('kfacq,spca->kpsfq', halfway, alpha_table(spread, row_index), precision=HIGHEST)
    weighted = spectrum.reshape(grid_size, grid_size, channels, spread) * quadrature(spread)[:, None, None, None]
    group_size = min(32, grid_size)
    group_count = grid_size // group_size
    grouped = jnp.transpose(weighted.reshape(grid_size, group_count, group_size, channels, spread), (1, 0, 2, 3, 4))
    row_groups = row_index.reshape(group_count, group_size)

    def map_group(group_pair):
        return degree_group(group_pair[0], group_pair[1], spread)
    coeffs = lax.map(map_group, (row_groups, grouped))
    coeffs = coeffs.reshape(grid_size, 2, functions, spread, spread)
    power = degree_energy(coeffs, spread)
    return (coeffs, power)
```

```python
import math

import jax
import jax.numpy as jnp
import numpy as np
from jax import lax
from jax.experimental import pallas as pl
from jax.experimental.pallas import tpu as pltpu
from jax.sharding import PartitionSpec as P

MESH = pl.DeviceIdType.MESH
F32 = jnp.float32
BF16 = jnp.bfloat16

GRID = 128
SPREAD = 64
FUNCTIONS = 4
CHANNELS = 8
DEVICES = 64
PLANES = 4
PLANE = 16
PLANE_ORDER = (0, 1, 3, 2)


def split_bf16(table):
    high = jnp.asarray(table, F32).astype(BF16)
    low = (jnp.asarray(table, F32) - high.astype(F32)).astype(BF16)
    return high, low


def fourier_tables():
    g = np.arange(GRID)
    q = np.arange(SPREAD)
    gamma = 2.0 * np.pi * ((g[:, None] * q[None, :]) % GRID) / GRID
    cosine, minus_sine = np.cos(gamma), -np.sin(gamma)
    first = np.concatenate([cosine, cosine, minus_sine, minus_sine], axis=1)
    j = np.arange(DEVICES)
    alpha = 2.0 * np.pi * ((2 * j[:, None] * g[None, :]) % GRID) / GRID
    c, s = np.cos(alpha) / GRID, np.sin(alpha) / GRID
    second = np.concatenate(
        [np.concatenate([c, s], axis=1), np.concatenate([-s, c], axis=1)], axis=0
    )
    packed = jnp.concatenate([*split_bf16(first), *split_bf16(second)], axis=0)
    turn = 2.0 * np.pi * g / GRID
    ones = np.ones((GRID, SPREAD))
    twist_cos = np.concatenate([ones, np.cos(turn)[:, None] * ones], axis=1)
    twist_sin = np.concatenate([0.0 * ones, np.sin(turn)[:, None] * ones], axis=1)
    return packed, twist_cos, twist_sin


def beta_tables():
    k = np.arange(GRID)
    angles = np.pi * (2 * k + 1) / 256.0
    odd = 2.0 * np.arange(SPREAD) + 1.0
    weight = (2.0 / SPREAD) * np.sin(angles)
    weight = weight * np.sum(np.sin(angles[:, None] * odd) / odd, axis=1)
    columns = [np.cos(angles), np.log(np.cos(angles / 2)), np.log(np.sin(angles / 2)), weight]
    return [np.repeat(column[:, None], GRID, axis=1) for column in columns]


def order_tables():
    lgamma = np.array([math.lgamma(v + 1.0) for v in range(2 * GRID + 1)])
    n = np.arange(GRID)
    p = np.where(n < SPREAD, n, n - GRID)[:, None]
    q = np.arange(SPREAD)[None, :]
    lowest = np.maximum(np.abs(p), q)
    t = np.maximum(0, q - p)
    magnitude = 0.5 * (
        lgamma[lowest + p] + lgamma[lowest - p] + lgamma[lowest + q] + lgamma[lowest - q]
    )
    magnitude = magnitude - lgamma[lowest + q - t] - lgamma[t]
    magnitude = magnitude - lgamma[p - q + t] - lgamma[lowest - p - t]
    sign = 1.0 - 2.0 * ((p - q + t) % 2)
    cos_power = 2 * lowest + q - p - 2 * t
    sin_power = p - q + 2 * t
    multiplicity = np.where(q == 0, 1.0, 2.0)
    rows = [magnitude, sign, cos_power, sin_power, lowest, p, q, multiplicity]
    rows = [np.broadcast_to(row, (GRID, SPREAD)).reshape(DEVICES, 1, 2 * SPREAD) for row in rows]
    return np.concatenate(rows, axis=1).astype(np.float32)


def row_slice(index):
    return pl.ds(pl.multiple_of(index * 16, 16), 16)


def body(
    samples_hbm,
    packed_hbm,
    real_hbm,
    order_hbm,
    coef_ref,
    power_ref,
    samples,
    packed,
    real,
    order,
    spectrum,
    received,
    wigner,
    total,
    forward_rows,
    cross_rows,
    backward_rows,
    shares,
    load_sem,
    send_sem,
    recv_sem,
    share_send_sem,
    share_recv_sem,
):
    me = lax.axis_index("beta")
    plane = me // PLANE
    within = me % PLANE

    def peer(offset):
        return (me + offset) % DEVICES

    barrier = pltpu.get_barrier_semaphore()

    def greet(offset, _):
        pl.semaphore_signal(
            barrier, 1, device_id={"beta": peer(offset)}, device_id_type=MESH
        )
        return 0

    lax.fori_loop(1, DEVICES, greet, 0)
    loads = [
        pltpu.make_async_copy(samples_hbm, samples, load_sem.at[0]),
        pltpu.make_async_copy(packed_hbm, packed, load_sem.at[1]),
        pltpu.make_async_copy(real_hbm, real, load_sem.at[2]),
        pltpu.make_async_copy(order_hbm.at[me], order, load_sem.at[3]),
    ]
    for load in loads:
        load.start()
    for load in loads:
        load.wait()

    def product(left, right):
        return jnp.dot(left, right, preferred_element_type=F32)

    def transform(k, _):
        values = samples[k].reshape(FUNCTIONS * GRID, GRID)
        high = values.astype(BF16)
        low = (values - high.astype(F32)).astype(BF16)
        gamma_high, gamma_low = packed[0:128, :], packed[128:256, :]
        halfway = product(high, gamma_high) + product(high, gamma_low) + product(low, gamma_high)
        twist_cos, twist_sin = real[0:128, :], real[128:256, :]
        alpha_high, alpha_low = packed[256:384, :], packed[384:512, :]
        for f in range(FUNCTIONS):
            part = halfway[f * GRID : (f + 1) * GRID]
            re, im = part[:, :128], part[:, 128:]
            turned = jnp.concatenate(
                [twist_cos * re + twist_sin * im, twist_cos * im - twist_sin * re], axis=0
            )
            turned_high = turned.astype(BF16)
            turned_low = (turned - turned_high.astype(F32)).astype(BF16)
            rows = (
                product(alpha_high, turned_high)
                + product(alpha_low, turned_high)
                + product(alpha_high, turned_low)
            )
            for s in range(2):
                spectrum[pl.ds(k * CHANNELS + s * FUNCTIONS + f, DEVICES, stride=16), :] = rows[
                    s * DEVICES : (s + 1) * DEVICES
                ]
        return 0

    lax.fori_loop(0, 2, transform, 0)

    pl.semaphore_wait(barrier, DEVICES - 1)

    def exchange(other):
        return pltpu.make_async_remote_copy(
            src_ref=spectrum.at[row_slice(other), :],
            dst_ref=received.at[row_slice(me), :],
            send_sem=send_sem.at[other],
            recv_sem=recv_sem.at[me],
            device_id={"beta": other},
            device_id_type=MESH,
        )

    def arrival(other):
        return pltpu.make_async_remote_copy(
            src_ref=spectrum.at[row_slice(other), :],
            dst_ref=received.at[row_slice(other), :],
            send_sem=send_sem.at[other],
            recv_sem=recv_sem.at[other],
            device_id={"beta": other},
            device_id_type=MESH,
        )

    for step in PLANE_ORDER:

        def send(r, _):
            other = (plane + step) % PLANES * PLANE + (within + r) % PLANE
            exchange(other).start()
            return 0

        lax.fori_loop(1 if step == 0 else 0, PLANE, send, 0)

    received[row_slice(me), :] = spectrum[row_slice(me), :]

    alpha_order, gamma_order = order[5:6, :], order[6:7, :]
    lowest = order[4:5, :]
    degree = lax.broadcasted_iota(jnp.int32, (SPREAD, 128), 0).astype(F32)
    previous = degree - 1.0
    upper = (degree * degree - alpha_order * alpha_order) * (
        degree * degree - gamma_order * gamma_order
    )
    lower = (previous * previous - alpha_order * alpha_order) * (
        previous * previous - gamma_order * gamma_order
    )
    root_upper = jnp.sqrt(jnp.maximum(upper, 1.0))
    forward = degree * (2.0 * previous + 1.0) / root_upper
    cross = alpha_order * gamma_order / jnp.maximum(previous * degree, 1.0)
    backward = (
        degree * jnp.sqrt(jnp.maximum(lower, 0.0)) / (jnp.maximum(previous, 1.0) * root_upper)
    )
    forward_rows[...] = forward
    cross_rows[...] = cross
    backward_rows[...] = backward

    cos_angles = real[256:384, :]
    start_value = (
        real[640:768, :]
        * order[1:2, :]
        * jnp.exp(
            order[0:1, :] + order[2:3, :] * real[384:512, :] + order[3:4, :] * real[512:640, :]
        )
    )
    real[384:512, :] = start_value

    half = GRID // 2
    for block in range(2):

        def advance(level, carried):
            former, current = carried
            f_row = forward_rows[pl.ds(level, 1), :]
            c_row = cross_rows[pl.ds(level, 1), :]
            b_row = backward_rows[pl.ds(level, 1), :]
            starts = lowest == level.astype(F32)
            cosine = real[256 + block * half : 256 + (block + 1) * half, :]
            first = real[384 + block * half : 384 + (block + 1) * half, :]
            recurred = f_row * (cosine - c_row) * current - b_row * former
            renewed = jnp.where(starts, first, recurred)
            wigner[pl.ds(pl.multiple_of(level * GRID + block * half, half), half), :] = renewed
            return current, renewed

        empty = cos_angles[:half] * 0.0
        lax.fori_loop(0, SPREAD, advance, (empty, empty))

    for position, step in enumerate(PLANE_ORDER):
        source = (plane + PLANES - step) % PLANES

        def await_one(r, _):
            arrival(source * PLANE + (within + r) % PLANE).wait_recv()
            return 0

        lax.fori_loop(1 if step == 0 else 0, PLANE, await_one, 0)

        def contract(block, _):
            rows = [pl.ds(pl.multiple_of(block * 64 + t * 8, 8), 8) for t in range(8)]
            if position == 0:
                sums = [jnp.zeros((8, 128), F32) for _ in range(8)]
            else:
                sums = [total[rows[t], :] for t in range(8)]
            for kk in range(32):
                k = source * 32 + kk
                values = received[pl.ds(pl.multiple_of(k * 8, 8), 8), :]
                for t in range(8):
                    factor = wigner[pl.ds((block * 8 + t) * GRID + k, 1), :]
                    sums[t] = sums[t] + values * factor
            for t in range(8):
                total[rows[t], :] = sums[t]
            return 0

        lax.fori_loop(0, 8, contract, 0)

    scale = 8.0 * jnp.sqrt(2.0 * degree + 1.0)
    coeffs = []
    for channel in range(CHANNELS):
        value = total[pl.ds(channel, SPREAD, stride=CHANNELS), :] * scale
        coef_ref[channel] = value
        coeffs.append(value)
    squares = jnp.concatenate(
        [coeffs[f] * coeffs[f] + coeffs[f + 4] * coeffs[f + 4] for f in range(FUNCTIONS)], axis=0
    )
    squares_high = squares.astype(BF16)
    squares_low = (squares - squares_high.astype(F32)).astype(BF16)
    multiplicity = jnp.broadcast_to(order[7:8, :], (16, 128)).astype(BF16)

    def lane_sum(values):
        return lax.dot_general(
            multiplicity, values, (((1,), (1,)), ((), ())), preferred_element_type=F32
        )

    energy = lane_sum(squares_high) + lane_sum(squares_low)
    lane = lax.broadcasted_iota(jnp.int32, (1, 128), 1)
    degrees = 2.0 * (lane % SPREAD).astype(F32) + 1.0
    inverse = 1.0 / (degrees * degrees)
    shares[me, 0:1, :] = energy[0:1, :128] * inverse
    shares[me, 1:2, :] = energy[0:1, 128:] * inverse

    def share(other):
        return pltpu.make_async_remote_copy(
            src_ref=shares.at[me],
            dst_ref=shares.at[me],
            send_sem=share_send_sem.at[other],
            recv_sem=share_recv_sem.at[me],
            device_id={"beta": other},
            device_id_type=MESH,
        )

    def share_arrival(other):
        return pltpu.make_async_remote_copy(
            src_ref=shares.at[other],
            dst_ref=shares.at[other],
            send_sem=share_send_sem.at[other],
            recv_sem=share_recv_sem.at[other],
            device_id={"beta": other},
            device_id_type=MESH,
        )

    def send_share(offset, _):
        share(peer(offset)).start()
        return 0

    def await_share(offset, _):
        share_arrival(peer(offset)).wait_recv()
        return 0

    def await_sent(offset, _):
        exchange(peer(offset)).wait_send()
        share(peer(offset)).wait_send()
        return 0

    lax.fori_loop(1, DEVICES, send_share, 0)
    lax.fori_loop(1, DEVICES, await_share, 0)

    result = shares[0]
    for index in range(1, DEVICES):
        result = result + shares[index]
    for f in range(FUNCTIONS):
        power_ref[f : f + 1, :] = result[f // 2 : f // 2 + 1, f % 2 * 64 : f % 2 * 64 + 64]
    lax.fori_loop(1, DEVICES, await_sent, 0)


def local(samples):
    packed, twist_cos, twist_sin = fourier_tables()
    real = jnp.asarray(np.concatenate([twist_cos, twist_sin, *beta_tables()], axis=0), F32)
    order = jnp.asarray(order_tables(), F32)
    hbm = pl.BlockSpec(memory_space=pl.ANY)
    vmem = pl.BlockSpec(memory_space=pltpu.VMEM)
    coef, power = pl.pallas_call(
        body,
        out_shape=(
            jax.ShapeDtypeStruct((CHANNELS, SPREAD, 128), F32),
            jax.ShapeDtypeStruct((FUNCTIONS, SPREAD), F32),
        ),
        in_specs=[hbm] * 4,
        out_specs=(vmem, vmem),
        scratch_shapes=[
            pltpu.VMEM((2, FUNCTIONS, GRID, GRID), F32),
            pltpu.VMEM((512, 256), BF16),
            pltpu.VMEM((768, 128), F32),
            pltpu.VMEM((8, 128), F32),
            pltpu.VMEM((DEVICES * 16, 128), F32),
            pltpu.VMEM((DEVICES * 16, 128), F32),
            pltpu.VMEM((SPREAD * GRID, 128), F32),
            pltpu.VMEM((SPREAD * CHANNELS, 128), F32),
            pltpu.VMEM((SPREAD, 128), F32),
            pltpu.VMEM((SPREAD, 128), F32),
            pltpu.VMEM((SPREAD, 128), F32),
            pltpu.VMEM((DEVICES, 2, 128), F32),
            pltpu.SemaphoreType.DMA((4,)),
            pltpu.SemaphoreType.DMA((DEVICES,)),
            pltpu.SemaphoreType.DMA((DEVICES,)),
            pltpu.SemaphoreType.DMA((DEVICES,)),
            pltpu.SemaphoreType.DMA((DEVICES,)),
        ],
        compiler_params=pltpu.CompilerParams(collective_id=0, has_side_effects=True),
        name="rotation_transform",
    )(samples, packed, real, order)
    coeffs = jnp.stack([coef[:, :, :SPREAD], coef[:, :, SPREAD:]], axis=0)
    return coeffs.reshape(2, 2, FUNCTIONS, SPREAD, SPREAD), power


def solution(mesh):
    return jax.shard_map(
        local,
        mesh=mesh,
        in_specs=(P("beta", "grp", None, None),),
        out_specs=(P("beta", None, "grp", None, None), P("grp", None)),
        check_vma=False,
    )
```

```python
import itertools
import math

import jax
import jax.numpy as jnp
import numpy as np
from jax import lax
from jax.experimental import pallas as pl
from jax.experimental.pallas import tpu as pltpu
from jax.sharding import PartitionSpec as P

MESH = pl.DeviceIdType.MESH
F32 = jnp.float32
BF16 = jnp.bfloat16

GRID = 128
SPREAD = 64
FUNCTIONS = 4
CHANNELS = 8
DEVICES = 64
PLANES = 4
PLANE = 16
RING_HOPS = (0, 1, 2, 1)


def hops(offset):
    return sum(RING_HOPS[step] for step in offset)


def far_first():
    near = sorted(
        (o for o in itertools.product(range(4), repeat=3) if o != (0, 0, 0)), key=hops
    )
    order = []
    for z, y, x in near:
        for turn in ((z, y, x), (y, x, z), (x, z, y)):
            for offset in (turn, tuple((4 - step) % 4 for step in turn)):
                if offset not in order:
                    order.append(offset)
    return order[::-1]


OFFSETS = far_first()
GROUPS = [
    [o for o in OFFSETS if hops(o) >= 4],
    [o for o in OFFSETS if hops(o) == 3],
    [o for o in OFFSETS if hops(o) == 2],
    [o for o in OFFSETS if hops(o) == 1],
]


def split_bf16(table):
    high = jnp.asarray(table, F32).astype(BF16)
    low = (jnp.asarray(table, F32) - high.astype(F32)).astype(BF16)
    return high, low


def fourier_tables():
    g = np.arange(GRID)
    q = np.arange(SPREAD)
    gamma = 2.0 * np.pi * ((g[:, None] * q[None, :]) % GRID) / GRID
    cosine, minus_sine = np.cos(gamma), -np.sin(gamma)
    first = np.concatenate([cosine, cosine, minus_sine, minus_sine], axis=1)
    j = np.arange(DEVICES)
    alpha = 2.0 * np.pi * ((2 * j[:, None] * g[None, :]) % GRID) / GRID
    c, s = np.cos(alpha) / GRID, np.sin(alpha) / GRID
    second = np.concatenate(
        [np.concatenate([c, s], axis=1), np.concatenate([-s, c], axis=1)], axis=0
    )
    packed = jnp.concatenate([*split_bf16(first), *split_bf16(second)], axis=0)
    turn = 2.0 * np.pi * g / GRID
    ones = np.ones((GRID, SPREAD))
    twist_cos = np.concatenate([ones, np.cos(turn)[:, None] * ones], axis=1)
    twist_sin = np.concatenate([0.0 * ones, np.sin(turn)[:, None] * ones], axis=1)
    return packed, twist_cos, twist_sin


def beta_tables():
    k = np.arange(GRID)
    angles = np.pi * (2 * k + 1) / 256.0
    odd = 2.0 * np.arange(SPREAD) + 1.0
    weight = (2.0 / SPREAD) * np.sin(angles)
    weight = weight * np.sum(np.sin(angles[:, None] * odd) / odd, axis=1)
    columns = [np.cos(angles), np.log(np.cos(angles / 2)), np.log(np.sin(angles / 2)), weight]
    return [np.repeat(column[:, None], GRID, axis=1) for column in columns]


def order_tables():
    lgamma = np.array([math.lgamma(v + 1.0) for v in range(2 * GRID + 1)])
    n = np.arange(GRID)
    p = np.where(n < SPREAD, n, n - GRID)[:, None]
    q = np.arange(SPREAD)[None, :]
    lowest = np.maximum(np.abs(p), q)
    t = np.maximum(0, q - p)
    magnitude = 0.5 * (
        lgamma[lowest + p] + lgamma[lowest - p] + lgamma[lowest + q] + lgamma[lowest - q]
    )
    magnitude = magnitude - lgamma[lowest + q - t] - lgamma[t]
    magnitude = magnitude - lgamma[p - q + t] - lgamma[lowest - p - t]
    sign = 1.0 - 2.0 * ((p - q + t) % 2)
    cos_power = 2 * lowest + q - p - 2 * t
    sin_power = p - q + 2 * t
    multiplicity = np.where(q == 0, 1.0, 2.0)
    rows = [magnitude, sign, cos_power, sin_power, lowest, p, q, multiplicity]
    rows = [np.broadcast_to(row, (GRID, SPREAD)).reshape(DEVICES, 1, 2 * SPREAD) for row in rows]
    return np.concatenate(rows, axis=1).astype(np.float32)


def row_slice(index):
    return pl.ds(pl.multiple_of(index * 16, 16), 16)


def body(
    samples_hbm,
    packed_hbm,
    real_hbm,
    order_hbm,
    coef_ref,
    power_ref,
    samples,
    packed,
    real,
    order,
    spectrum,
    received,
    wigner,
    total,
    forward_rows,
    cross_rows,
    backward_rows,
    shares,
    load_sem,
    send_sem,
    recv_sem,
):
    me = lax.axis_index("beta")
    place = (me // 16, me // 4 % 4, me % 4)

    def target(offset):
        z, y, x = ((place[axis] + offset[axis]) % 4 for axis in range(3))
        return z * 16 + y * 4 + x

    def origin(offset):
        return target(tuple((4 - step) % 4 for step in offset))

    loads = [
        pltpu.make_async_copy(samples_hbm, samples, load_sem.at[0]),
        pltpu.make_async_copy(packed_hbm, packed, load_sem.at[1]),
        pltpu.make_async_copy(real_hbm, real, load_sem.at[2]),
        pltpu.make_async_copy(order_hbm.at[me], order, load_sem.at[3]),
    ]
    for load in loads:
        load.start()

    barrier = pltpu.get_barrier_semaphore()
    with jax.named_scope("greet"):
        for offset in OFFSETS:
            pl.semaphore_signal(
                barrier, 1, device_id={"beta": target(offset)}, device_id_type=MESH
            )

    with jax.named_scope("load"):
        for load in loads:
            load.wait()

    def product(left, right):
        return jnp.dot(left, right, preferred_element_type=F32)

    def transform(k, _):
        values = samples[k].reshape(FUNCTIONS * GRID, GRID)
        high = values.astype(BF16)
        low = (values - high.astype(F32)).astype(BF16)
        gamma_high, gamma_low = packed[0:128, :], packed[128:256, :]
        halfway = product(high, gamma_high) + product(high, gamma_low) + product(low, gamma_high)
        twist_cos, twist_sin = real[0:128, :], real[128:256, :]
        alpha_high, alpha_low = packed[256:384, :], packed[384:512, :]
        for f in range(FUNCTIONS):
            part = halfway[f * GRID : (f + 1) * GRID]
            re, im = part[:, :128], part[:, 128:]
            turned = jnp.concatenate(
                [twist_cos * re + twist_sin * im, twist_cos * im - twist_sin * re], axis=0
            )
            turned_high = turned.astype(BF16)
            turned_low = (turned - turned_high.astype(F32)).astype(BF16)
            rows = (
                product(alpha_high, turned_high)
                + product(alpha_low, turned_high)
                + product(alpha_high, turned_low)
            )
            for s in range(2):
                spectrum[pl.ds(k * CHANNELS + s * FUNCTIONS + f, DEVICES, stride=16), :] = rows[
                    s * DEVICES : (s + 1) * DEVICES
                ]
        return 0

    with jax.named_scope("dft"):
        lax.fori_loop(0, 2, transform, 0)

    with jax.named_scope("barrier_wait"):
        pl.semaphore_wait(barrier, DEVICES - 1)

    with jax.named_scope("send"):
        for group, members in enumerate(GROUPS):
            for offset in members:
                other = target(offset)
                pltpu.make_async_remote_copy(
                    src_ref=spectrum.at[row_slice(other), :],
                    dst_ref=received.at[row_slice(me), :],
                    send_sem=send_sem.at[0],
                    recv_sem=recv_sem.at[group],
                    device_id={"beta": other},
                    device_id_type=MESH,
                ).start()

    def await_group(group):
        count = len(GROUPS[group])
        pltpu.make_async_remote_copy(
            src_ref=spectrum.at[0 : count * 16, :],
            dst_ref=received.at[0 : count * 16, :],
            send_sem=send_sem.at[0],
            recv_sem=recv_sem.at[group],
            device_id={"beta": target(OFFSETS[0])},
            device_id_type=MESH,
        ).wait_recv()

    received[row_slice(me), :] = spectrum[row_slice(me), :]

    with jax.named_scope("coeff"):
        alpha_order, gamma_order = order[5:6, :], order[6:7, :]
        lowest = order[4:5, :]
        degree = lax.broadcasted_iota(jnp.int32, (SPREAD, 128), 0).astype(F32)
        previous = degree - 1.0
        upper = (degree * degree - alpha_order * alpha_order) * (
            degree * degree - gamma_order * gamma_order
        )
        lower = (previous * previous - alpha_order * alpha_order) * (
            previous * previous - gamma_order * gamma_order
        )
        root_upper = jnp.sqrt(jnp.maximum(upper, 1.0))
        forward = degree * (2.0 * previous + 1.0) / root_upper
        cross = alpha_order * gamma_order / jnp.maximum(previous * degree, 1.0)
        backward = (
            degree * jnp.sqrt(jnp.maximum(lower, 0.0)) / (jnp.maximum(previous, 1.0) * root_upper)
        )
        forward_rows[...] = forward
        cross_rows[...] = cross
        backward_rows[...] = backward

        cos_angles = real[256:384, :]
        start_value = (
            real[640:768, :]
            * order[1:2, :]
            * jnp.exp(
                order[0:1, :] + order[2:3, :] * real[384:512, :] + order[3:4, :] * real[512:640, :]
            )
        )
        real[384:512, :] = start_value

    half = GRID // 2
    with jax.named_scope("wigner"):
        for block in range(2):

            def advance(level, carried):
                former, current = carried
                f_row = forward_rows[pl.ds(level, 1), :]
                c_row = cross_rows[pl.ds(level, 1), :]
                b_row = backward_rows[pl.ds(level, 1), :]
                starts = lowest == level.astype(F32)
                cosine = real[256 + block * half : 256 + (block + 1) * half, :]
                first = real[384 + block * half : 384 + (block + 1) * half, :]
                recurred = f_row * (cosine - c_row) * current - b_row * former
                renewed = jnp.where(starts, first, recurred)
                wigner[pl.ds(pl.multiple_of(level * GRID + block * half, half), half), :] = renewed
                return current, renewed

            empty = cos_angles[:half] * 0.0
            lax.fori_loop(0, SPREAD, advance, (empty, empty))

    for group, members in enumerate(GROUPS):
        with jax.named_scope(f"wait{group}"):
            await_group(group)
        sources = [origin(offset) for offset in members]
        if group == 0:
            sources = [me] + sources

        def contract(block, _):
            rows = [pl.ds(pl.multiple_of(block * 64 + t * 8, 8), 8) for t in range(8)]
            if group == 0:
                sums = [jnp.zeros((8, 128), F32) for _ in range(8)]
            else:
                sums = [total[rows[t], :] for t in range(8)]
            for source in sources:
                for kk in range(2):
                    k = source * 2 + kk
                    values = received[pl.ds(pl.multiple_of(k * 8, 8), 8), :]
                    for t in range(8):
                        factor = wigner[pl.ds((block * 8 + t) * GRID + k, 8, stride=0), :]
                        sums[t] = sums[t] + values * factor
            for t in range(8):
                total[rows[t], :] = sums[t]
            return 0

        with jax.named_scope(f"contract{group}"):
            lax.fori_loop(0, 8, contract, 0)

    with jax.named_scope("finish"):
        scale = 8.0 * jnp.sqrt(2.0 * degree + 1.0)
        coeffs = []
        for channel in range(CHANNELS):
            value = total[pl.ds(channel, SPREAD, stride=CHANNELS), :] * scale
            coeffs.append(value)
        squares = jnp.concatenate(
            [coeffs[f] * coeffs[f] + coeffs[f + 4] * coeffs[f + 4] for f in range(FUNCTIONS)], axis=0
        )
        squares_high = squares.astype(BF16)
        squares_low = (squares - squares_high.astype(F32)).astype(BF16)
        multiplicity = jnp.broadcast_to(order[7:8, :], (16, 128)).astype(BF16)

        def lane_sum(values):
            return lax.dot_general(
                multiplicity, values, (((1,), (1,)), ((), ())), preferred_element_type=F32
            )

        energy = lane_sum(squares_high) + lane_sum(squares_low)
        lane = lax.broadcasted_iota(jnp.int32, (1, 128), 1)
        degrees = 2.0 * (lane % SPREAD).astype(F32) + 1.0
        inverse = 1.0 / (degrees * degrees)
        shares[me, 0:1, :] = energy[0:1, :128] * inverse
        shares[me, 1:2, :] = energy[0:1, 128:] * inverse

    with jax.named_scope("share_send"):
        for offset in OFFSETS:
            pltpu.make_async_remote_copy(
                src_ref=shares.at[me],
                dst_ref=shares.at[me],
                send_sem=send_sem.at[1],
                recv_sem=recv_sem.at[len(GROUPS)],
                device_id={"beta": target(offset)},
                device_id_type=MESH,
            ).start()

    with jax.named_scope("store"):
        for channel in range(CHANNELS):
            coef_ref[0, channel] = coeffs[channel][:, :SPREAD]
            coef_ref[1, channel] = coeffs[channel][:, SPREAD:]

    others = DEVICES - 1
    with jax.named_scope("sent"):
        pltpu.make_async_remote_copy(
            src_ref=spectrum.at[0 : others * 16, :],
            dst_ref=received.at[0 : others * 16, :],
            send_sem=send_sem.at[0],
            recv_sem=recv_sem.at[0],
            device_id={"beta": target(OFFSETS[0])},
            device_id_type=MESH,
        ).wait_send()

    with jax.named_scope("share_wait"):
        shared = pltpu.make_async_remote_copy(
            src_ref=shares.at[0:others],
            dst_ref=shares.at[0:others],
            send_sem=send_sem.at[1],
            recv_sem=recv_sem.at[len(GROUPS)],
            device_id={"beta": target(OFFSETS[0])},
            device_id_type=MESH,
        )
        shared.wait_send()
        shared.wait_recv()

    with jax.named_scope("share_sum"):
        result = shares[0]
        for index in range(1, DEVICES):
            result = result + shares[index]
        for f in range(FUNCTIONS):
            power_ref[f : f + 1, :] = result[f // 2 : f // 2 + 1, f % 2 * 64 : f % 2 * 64 + 64]


def local(samples):
    packed, twist_cos, twist_sin = fourier_tables()
    real = jnp.asarray(np.concatenate([twist_cos, twist_sin, *beta_tables()], axis=0), F32)
    order = jnp.asarray(order_tables(), F32)
    hbm = pl.BlockSpec(memory_space=pl.ANY)
    vmem = pl.BlockSpec(memory_space=pltpu.VMEM)
    coef, power = pl.pallas_call(
        body,
        out_shape=(
            pltpu.VMEM((2, CHANNELS, SPREAD, SPREAD), F32),
            pltpu.VMEM((FUNCTIONS, SPREAD), F32),
        ),
        in_specs=[hbm] * 4,
        out_specs=(vmem, vmem),
        scratch_shapes=[
            pltpu.VMEM((2, FUNCTIONS, GRID, GRID), F32),
            pltpu.VMEM((512, 256), BF16),
            pltpu.VMEM((768, 128), F32),
            pltpu.VMEM((8, 128), F32),
            pltpu.VMEM((DEVICES * 16, 128), F32),
            pltpu.VMEM((DEVICES * 16, 128), F32),
            pltpu.VMEM((SPREAD * GRID, 128), F32),
            pltpu.VMEM((SPREAD * CHANNELS, 128), F32),
            pltpu.VMEM((SPREAD, 128), F32),
            pltpu.VMEM((SPREAD, 128), F32),
            pltpu.VMEM((SPREAD, 128), F32),
            pltpu.VMEM((DEVICES, 2, 128), F32),
            pltpu.SemaphoreType.DMA((4,)),
            pltpu.SemaphoreType.DMA((2,)),
            pltpu.SemaphoreType.DMA((len(GROUPS) + 1,)),
        ],
        compiler_params=pltpu.CompilerParams(collective_id=0, has_side_effects=True),
        name="rotation_transform",
    )(samples, packed, real, order)
    return coef.reshape(2, 2, FUNCTIONS, SPREAD, SPREAD), power


def solution(mesh):
    return jax.shard_map(
        local,
        mesh=mesh,
        in_specs=(P("beta", "grp", None, None),),
        out_specs=(P("beta", None, "grp", None, None), P("grp", None)),
        check_vma=False,
    )
```

```python
import itertools
import math

import jax
import jax.numpy as jnp
import numpy as np
from jax import lax
from jax.experimental import pallas as pl
from jax.experimental.pallas import tpu as pltpu
from jax.sharding import PartitionSpec as P

MESH = pl.DeviceIdType.MESH
F32 = jnp.float32
BF16 = jnp.bfloat16

GRID = 128
SPREAD = 64
FUNCTIONS = 4
CHANNELS = 8
DEVICES = 64
OTHERS = DEVICES - 1
HALF = DEVICES * CHANNELS
RING_HOPS = (0, 1, 2, 1)


def hops(offset):
    return sum(RING_HOPS[step] for step in offset)


def far_first():
    near = sorted(
        (o for o in itertools.product(range(4), repeat=3) if o != (0, 0, 0)), key=hops
    )
    order = []
    for z, y, x in near:
        for turn in ((z, y, x), (y, x, z), (x, z, y)):
            for offset in (turn, tuple((4 - step) % 4 for step in turn)):
                if offset not in order:
                    order.append(offset)
    return order[::-1]


OFFSETS = far_first()


def split_bf16(table):
    high = jnp.asarray(table, F32).astype(BF16)
    low = (jnp.asarray(table, F32) - high.astype(F32)).astype(BF16)
    return high, low


def fourier_tables():
    g = np.arange(GRID)
    q = np.arange(SPREAD)
    gamma = 2.0 * np.pi * ((g[:, None] * q[None, :]) % GRID) / GRID
    cosine, minus_sine = np.cos(gamma), -np.sin(gamma)
    first = np.concatenate([cosine, cosine, minus_sine, minus_sine], axis=1)
    j = np.arange(DEVICES)
    alpha = 2.0 * np.pi * ((2 * j[:, None] * g[None, :]) % GRID) / GRID
    c, s = np.cos(alpha) / GRID, np.sin(alpha) / GRID
    second = np.concatenate(
        [np.concatenate([c, s], axis=1), np.concatenate([-s, c], axis=1)], axis=0
    )
    first_high, first_low = split_bf16(first)
    packed = jnp.concatenate([first_high, first_high, first_low, *split_bf16(second)], axis=0)
    turn = 2.0 * np.pi * g / GRID
    ones = np.ones((GRID, SPREAD))
    twist_cos = np.concatenate([ones, np.cos(turn)[:, None] * ones], axis=1)
    twist_sin = np.concatenate([0.0 * ones, np.sin(turn)[:, None] * ones], axis=1)
    return packed, jnp.asarray(np.concatenate([twist_cos, twist_sin], axis=0), F32)


def beta_tables():
    k = np.arange(GRID).reshape(DEVICES, 2).T.reshape(GRID)
    angles = np.pi * (2 * k + 1) / 256.0
    odd = 2.0 * np.arange(SPREAD) + 1.0
    weight = (2.0 / SPREAD) * np.sin(angles)
    weight = weight * np.sum(np.sin(angles[:, None] * odd) / odd, axis=1)
    columns = [np.cos(angles), np.log(np.cos(angles / 2)), np.log(np.sin(angles / 2)), weight]
    tables = [np.repeat(column[:, None], GRID, axis=1) for column in columns]
    return jnp.asarray(np.concatenate(tables, axis=0), F32)


def order_tables():
    lgamma = np.array([math.lgamma(v + 1.0) for v in range(2 * GRID + 1)])
    n = np.arange(GRID)
    p = np.where(n < SPREAD, n, n - GRID)[:, None]
    q = np.arange(SPREAD)[None, :]
    lowest = np.maximum(np.abs(p), q)
    t = np.maximum(0, q - p)
    magnitude = 0.5 * (
        lgamma[lowest + p] + lgamma[lowest - p] + lgamma[lowest + q] + lgamma[lowest - q]
    )
    magnitude = magnitude - lgamma[lowest + q - t] - lgamma[t]
    magnitude = magnitude - lgamma[p - q + t] - lgamma[lowest - p - t]
    sign = 1.0 - 2.0 * ((p - q + t) % 2)
    cos_power = 2 * lowest + q - p - 2 * t
    sin_power = p - q + 2 * t
    multiplicity = np.where(q == 0, 1.0, 2.0)
    rows = [magnitude, sign, cos_power, sin_power, lowest, p, q, multiplicity]
    rows = [np.broadcast_to(row, (GRID, SPREAD)).reshape(DEVICES, 1, 2 * SPREAD) for row in rows]
    return jnp.asarray(np.concatenate(rows, axis=1), F32)


def slot(offset):
    return offset[0] * 16 + offset[1] * 4 + offset[2]


def tile(index):
    return pl.ds(pl.multiple_of(index * 8, 8), 8)


def body(
    samples_hbm,
    packed_hbm,
    twist_hbm,
    beta_hbm,
    order_hbm,
    coef_ref,
    shares,
    samples,
    packed,
    twist,
    beta,
    order,
    spectrum,
    received,
    wigner,
    total,
    rows_of_level,
    placed,
    load_sem,
    send_sem,
    recv_sem,
):
    me = lax.axis_index("beta")
    place = (me // 16, me // 4 % 4, me % 4)

    def target(offset):
        z, y, x = ((place[axis] + offset[axis]) % 4 for axis in range(3))
        return z * 16 + y * 4 + x

    loads = [
        pltpu.make_async_copy(packed_hbm, packed, load_sem.at[0]),
        pltpu.make_async_copy(samples_hbm.at[0], samples.at[0], load_sem.at[1]),
        pltpu.make_async_copy(twist_hbm, twist, load_sem.at[2]),
        pltpu.make_async_copy(samples_hbm.at[1], samples.at[1], load_sem.at[3]),
        pltpu.make_async_copy(beta_hbm, beta, load_sem.at[4]),
        pltpu.make_async_copy(order_hbm.at[me], order, load_sem.at[5]),
    ]
    for load in loads:
        load.start()

    barrier = pltpu.get_barrier_semaphore()
    with jax.named_scope("greet"):
        for offset in OFFSETS:
            pl.semaphore_signal(
                barrier, 1, device_id={"beta": target(offset)}, device_id_type=MESH
            )

    def product(left, right):
        return jnp.dot(left, right, preferred_element_type=F32)

    def split(values):
        high = values.astype(BF16)
        return high, (values - high.astype(F32)).astype(BF16)

    def transform(k):
        high, low = split(samples[k].reshape(FUNCTIONS * GRID, GRID))
        halfway = product(jnp.concatenate([high, low], axis=1), packed[0:256, :])
        halfway = halfway + product(high, packed[256:384, :])
        twist_cos, twist_sin = twist[0:128, :], twist[128:256, :]
        alpha_high, alpha_low = packed[384:512, :], packed[512:640, :]
        for pair in range(2):
            turned = []
            for f in (2 * pair, 2 * pair + 1):
                part = halfway[f * GRID : (f + 1) * GRID]
                re, im = part[:, :128], part[:, 128:]
                turned.append(
                    jnp.concatenate(
                        [twist_cos * re + twist_sin * im, twist_cos * im - twist_sin * re], axis=0
                    )
                )
            turned_high, turned_low = split(jnp.concatenate(turned, axis=1))
            rows = (
                product(alpha_high, turned_high)
                + product(alpha_low, turned_high)
                + product(alpha_high, turned_low)
            )
            for s in range(2):
                for f in range(2):
                    spectrum[
                        pl.ds(k * HALF + s * FUNCTIONS + 2 * pair + f, DEVICES, stride=8), :
                    ] = rows[s * DEVICES : (s + 1) * DEVICES, f * 128 : (f + 1) * 128]

    def send(k):
        for offset in OFFSETS:
            other = target(offset)
            pltpu.make_async_remote_copy(
                src_ref=spectrum.at[tile(k * DEVICES + other), :],
                dst_ref=received.at[pl.ds(k * HALF + slot(offset) * 8, 8), :],
                send_sem=send_sem.at[0],
                recv_sem=recv_sem.at[k],
                device_id={"beta": other},
                device_id_type=MESH,
            ).start()

    with jax.named_scope("load"):
        for load in loads[:3]:
            load.wait()
    with jax.named_scope("dft0"):
        transform(0)
    with jax.named_scope("barrier_wait"):
        pl.semaphore_wait(barrier, OTHERS)
    with jax.named_scope("send0"):
        send(0)
    with jax.named_scope("load1"):
        for load in loads[3:]:
            load.wait()
    with jax.named_scope("dft1"):
        transform(1)
    with jax.named_scope("send1"):
        send(1)
    for k in range(2):
        received[k * HALF : k * HALF + 8, :] = spectrum[tile(k * DEVICES + me), :]

    with jax.named_scope("coeff"):
        alpha_order, gamma_order = order[5:6, :], order[6:7, :]
        lowest = order[4:5, :]
        degree = lax.broadcasted_iota(jnp.int32, (SPREAD, 128), 0).astype(F32)
        previous = degree - 1.0
        upper = (degree * degree - alpha_order * alpha_order) * (
            degree * degree - gamma_order * gamma_order
        )
        lower = (previous * previous - alpha_order * alpha_order) * (
            previous * previous - gamma_order * gamma_order
        )
        root_upper = jnp.sqrt(jnp.maximum(upper, 1.0))
        rows_of_level[0] = degree * (2.0 * previous + 1.0) / root_upper
        rows_of_level[1] = alpha_order * gamma_order / jnp.maximum(previous * degree, 1.0)
        rows_of_level[2] = (
            degree * jnp.sqrt(jnp.maximum(lower, 0.0)) / (jnp.maximum(previous, 1.0) * root_upper)
        )
        beta[128:256, :] = (
            beta[384:512, :]
            * order[1:2, :]
            * jnp.exp(
                order[0:1, :] + order[2:3, :] * beta[128:256, :] + order[3:4, :] * beta[256:384, :]
            )
        )

        def arrange(index, _):
            z = (place[0] + 4 - index // 16) % 4
            y = (place[1] + 4 - index // 4 % 4) % 4
            x = (place[2] + 4 - index % 4) % 4
            sender = z * 16 + y * 4 + x
            for k in range(2):
                for table in range(2):
                    placed[table, pl.ds(k * DEVICES + index, 1), :] = beta[
                        pl.ds(table * GRID + k * DEVICES + sender, 1), :
                    ]
            return 0

        lax.fori_loop(0, DEVICES, arrange, 0, unroll=4)

    with jax.named_scope("wigner"):
        for k in range(2):

            def advance(level, carried):
                former, current = carried
                f_row = rows_of_level[0, pl.ds(level, 1), :]
                c_row = rows_of_level[1, pl.ds(level, 1), :]
                b_row = rows_of_level[2, pl.ds(level, 1), :]
                starts = lowest == level.astype(F32)
                cosine = placed[0, k * DEVICES : (k + 1) * DEVICES, :]
                first = placed[1, k * DEVICES : (k + 1) * DEVICES, :]
                recurred = f_row * (cosine - c_row) * current - b_row * former
                renewed = jnp.where(starts, first, recurred)
                wigner[pl.ds(pl.multiple_of(level * GRID + k * DEVICES, 64), DEVICES), :] = renewed
                return current, renewed

            empty = placed[0, 0:DEVICES, :] * 0.0
            lax.fori_loop(0, SPREAD, advance, (empty, empty))

    for k in range(2):
        with jax.named_scope(f"wait{k}"):
            pltpu.make_async_remote_copy(
                src_ref=spectrum.at[0 : OTHERS * 8, :],
                dst_ref=received.at[0 : OTHERS * 8, :],
                send_sem=send_sem.at[0],
                recv_sem=recv_sem.at[k],
                device_id={"beta": target(OFFSETS[0])},
                device_id_type=MESH,
            ).wait_recv()

        def contract(block, _):
            rows = [pl.ds(pl.multiple_of(block * 128 + t * 8, 8), 8) for t in range(16)]
            if k == 0:
                sums = tuple(rows_of_level[0, 0:8, :] * 0.0 for _ in range(16))
            else:
                sums = tuple(total[rows[t], :] for t in range(16))

            def gather(group, sums):
                sums = list(sums)
                base = group * 16
                for index in range(16):
                    values = received[pl.ds(pl.multiple_of(base * 8, 8) + k * HALF + index * 8, 8), :]
                    for t in range(16):
                        factor = wigner[
                            pl.ds(
                                block * 16 * GRID + base + (t * GRID + k * DEVICES + index),
                                8,
                                stride=0,
                            ),
                            :,
                        ]
                        sums[t] = sums[t] + values * factor
                return tuple(sums)

            sums = lax.fori_loop(0, 4, gather, sums)
            for t in range(16):
                total[rows[t], :] = sums[t]
            return 0

        with jax.named_scope(f"contract{k}"):
            lax.fori_loop(0, 4, contract, 0)

    with jax.named_scope("finish"):
        scale = 8.0 * jnp.sqrt(2.0 * degree + 1.0)
        coeffs = []
        for channel in range(CHANNELS):
            coeffs.append(total[pl.ds(channel, SPREAD, stride=CHANNELS), :] * scale)
        squares = jnp.concatenate(
            [coeffs[f] * coeffs[f] + coeffs[f + 4] * coeffs[f + 4] for f in range(FUNCTIONS)], axis=0
        )
        squares_high, squares_low = split(squares)
        multiplicity = jnp.broadcast_to(order[7:8, :], (16, 128)).astype(BF16)

        def lane_sum(values):
            return lax.dot_general(
                multiplicity, values, (((1,), (1,)), ((), ())), preferred_element_type=F32
            )

        energy = lane_sum(squares_high) + lane_sum(squares_low)
        lane = lax.broadcasted_iota(jnp.int32, (1, 128), 1)
        degrees = 2.0 * (lane % SPREAD).astype(F32) + 1.0
        inverse = 1.0 / (degrees * degrees)
        shares[me, 0:1, :] = energy[0:1, :128] * inverse
        shares[me, 1:2, :] = energy[0:1, 128:] * inverse

    with jax.named_scope("share_send"):
        for offset in OFFSETS:
            pltpu.make_async_remote_copy(
                src_ref=shares.at[me],
                dst_ref=shares.at[me],
                send_sem=send_sem.at[1],
                recv_sem=recv_sem.at[2],
                device_id={"beta": target(offset)},
                device_id_type=MESH,
            ).start()

    with jax.named_scope("store"):
        for channel in range(CHANNELS):
            coef_ref[0, channel] = coeffs[channel][:, :SPREAD]
            coef_ref[1, channel] = coeffs[channel][:, SPREAD:]

    with jax.named_scope("sent"):
        for k in range(2):
            pltpu.make_async_remote_copy(
                src_ref=spectrum.at[0 : OTHERS * 8, :],
                dst_ref=received.at[0 : OTHERS * 8, :],
                send_sem=send_sem.at[0],
                recv_sem=recv_sem.at[0],
                device_id={"beta": target(OFFSETS[0])},
                device_id_type=MESH,
            ).wait_send()

    with jax.named_scope("share_wait"):
        shared = pltpu.make_async_remote_copy(
            src_ref=shares.at[0:OTHERS],
            dst_ref=shares.at[0:OTHERS],
            send_sem=send_sem.at[1],
            recv_sem=recv_sem.at[2],
            device_id={"beta": target(OFFSETS[0])},
            device_id_type=MESH,
        )
        shared.wait_send()
        shared.wait_recv()


def tail(coef_ref, shares, coef_hbm, power_hbm, power, sem):
    store = pltpu.make_async_copy(coef_ref, coef_hbm, sem.at[0])
    store.start()
    sums = [shares[index] for index in range(4)]
    for index in range(4, DEVICES):
        sums[index % 4] = sums[index % 4] + shares[index]
    result = (sums[0] + sums[1]) + (sums[2] + sums[3])
    for f in range(FUNCTIONS):
        power[f : f + 1, :] = result[f // 2 : f // 2 + 1, f % 2 * 64 : f % 2 * 64 + 64]
    finish = pltpu.make_async_copy(power, power_hbm, sem.at[1])
    finish.start()
    store.wait()
    finish.wait()


def local(samples):
    packed, twist = fourier_tables()
    anywhere = pl.BlockSpec(memory_space=pl.ANY)
    vmem = pl.BlockSpec(memory_space=pltpu.VMEM)
    coef, shares = pl.pallas_call(
        body,
        out_shape=(
            pltpu.VMEM((2, CHANNELS, SPREAD, SPREAD), F32),
            pltpu.VMEM((DEVICES, 2, 128), F32),
        ),
        in_specs=[anywhere] * 5,
        out_specs=(vmem, vmem),
        scratch_shapes=[
            pltpu.VMEM((2, FUNCTIONS, GRID, GRID), F32),
            pltpu.VMEM((640, 256), BF16),
            pltpu.VMEM((256, 128), F32),
            pltpu.VMEM((512, 128), F32),
            pltpu.VMEM((8, 128), F32),
            pltpu.VMEM((2 * HALF, 128), F32),
            pltpu.VMEM((2 * HALF, 128), F32),
            pltpu.VMEM((SPREAD * GRID, 128), F32),
            pltpu.VMEM((SPREAD * CHANNELS, 128), F32),
            pltpu.VMEM((3, SPREAD, 128), F32),
            pltpu.VMEM((2, GRID, 128), F32),
            pltpu.SemaphoreType.DMA((6,)),
            pltpu.SemaphoreType.DMA((2,)),
            pltpu.SemaphoreType.DMA((3,)),
        ],
        compiler_params=pltpu.CompilerParams(collective_id=0, has_side_effects=True),
        name="rotation_transform",
    )(samples, packed, twist, beta_tables(), order_tables())
    coef, power = pl.pallas_call(
        tail,
        out_shape=(
            jax.ShapeDtypeStruct((2, CHANNELS, SPREAD, SPREAD), F32),
            jax.ShapeDtypeStruct((FUNCTIONS, SPREAD), F32),
        ),
        in_specs=[vmem, vmem],
        out_specs=(anywhere, anywhere),
        scratch_shapes=[pltpu.VMEM((FUNCTIONS, SPREAD), F32), pltpu.SemaphoreType.DMA((2,))],
        compiler_params=pltpu.CompilerParams(vmem_limit_bytes=4 * 1024 * 1024),
        name="store_results",
    )(coef, shares)
    return coef.reshape(2, 2, FUNCTIONS, SPREAD, SPREAD), power


def solution(mesh):
    return jax.shard_map(
        local,
        mesh=mesh,
        in_specs=(P("beta", "grp", None, None),),
        out_specs=(P("beta", None, "grp", None, None), P("grp", None)),
        check_vma=False,
    )
```

```python
import itertools
import math

import jax
import jax.numpy as jnp
import numpy as np
from jax import lax
from jax.experimental import pallas as pl
from jax.experimental.pallas import tpu as pltpu
from jax.sharding import PartitionSpec as P

MESH = pl.DeviceIdType.MESH
F32 = jnp.float32
BF16 = jnp.bfloat16

GRID = 128
SPREAD = 64
FUNCTIONS = 4
CHANNELS = 8
DEVICES = 64
OTHERS = DEVICES - 1
HALF = DEVICES * CHANNELS
RING_HOPS = (0, 1, 2, 1)


def hops(offset):
    return sum(RING_HOPS[step] for step in offset)


def far_first():
    near = sorted(
        (o for o in itertools.product(range(4), repeat=3) if o != (0, 0, 0)), key=hops
    )
    order = []
    for z, y, x in near:
        for turn in ((z, y, x), (y, x, z), (x, z, y)):
            for offset in (turn, tuple((4 - step) % 4 for step in turn)):
                if offset not in order:
                    order.append(offset)
    return order[::-1]


OFFSETS = far_first()
CHUNKS = (((0, 64),), ((0, 32), (32, 48), (48, 64)), ((0, 64),))


def split_bf16(table):
    high = jnp.asarray(table, F32).astype(BF16)
    low = (jnp.asarray(table, F32) - high.astype(F32)).astype(BF16)
    return high, low


def fourier_tables():
    g = np.arange(GRID)
    q = np.arange(SPREAD)
    gamma = 2.0 * np.pi * ((g[:, None] * q[None, :]) % GRID) / GRID
    cosine, minus_sine = np.cos(gamma), -np.sin(gamma)
    first = np.concatenate([cosine, cosine, minus_sine, minus_sine], axis=1)
    j = np.arange(DEVICES)
    alpha = 2.0 * np.pi * ((2 * j[:, None] * g[None, :]) % GRID) / GRID
    c, s = np.cos(alpha) / GRID, np.sin(alpha) / GRID
    second = np.concatenate(
        [np.concatenate([c, s], axis=1), np.concatenate([-s, c], axis=1)], axis=0
    )
    first_high, first_low = split_bf16(first)
    packed = jnp.concatenate([first_high, first_high, first_low, *split_bf16(second)], axis=0)
    turn = 2.0 * np.pi * g / GRID
    ones = np.ones((GRID, SPREAD))
    twist_cos = np.concatenate([ones, np.cos(turn)[:, None] * ones], axis=1)
    twist_sin = np.concatenate([0.0 * ones, np.sin(turn)[:, None] * ones], axis=1)
    return packed, jnp.asarray(np.concatenate([twist_cos, twist_sin], axis=0), F32)


def beta_tables():
    k = np.arange(GRID).reshape(DEVICES, 2).T.reshape(GRID)
    angles = np.pi * (2 * k + 1) / 256.0
    odd = 2.0 * np.arange(SPREAD) + 1.0
    weight = (2.0 / SPREAD) * np.sin(angles)
    weight = weight * np.sum(np.sin(angles[:, None] * odd) / odd, axis=1)
    columns = [np.cos(angles), np.log(np.cos(angles / 2)), np.log(np.sin(angles / 2)), weight]
    tables = [np.repeat(column[:, None], GRID, axis=1) for column in columns]
    return jnp.asarray(np.concatenate(tables, axis=0), F32)


def order_tables():
    lgamma = np.array([math.lgamma(v + 1.0) for v in range(2 * GRID + 1)])
    n = np.arange(GRID)
    p = np.where(n < SPREAD, n, n - GRID)[:, None]
    q = np.arange(SPREAD)[None, :]
    lowest = np.maximum(np.abs(p), q)
    t = np.maximum(0, q - p)
    magnitude = 0.5 * (
        lgamma[lowest + p] + lgamma[lowest - p] + lgamma[lowest + q] + lgamma[lowest - q]
    )
    magnitude = magnitude - lgamma[lowest + q - t] - lgamma[t]
    magnitude = magnitude - lgamma[p - q + t] - lgamma[lowest - p - t]
    sign = 1.0 - 2.0 * ((p - q + t) % 2)
    cos_power = 2 * lowest + q - p - 2 * t
    sin_power = p - q + 2 * t
    multiplicity = np.where(q == 0, 1.0, 2.0)
    rows = [magnitude, sign, cos_power, sin_power, lowest, p, q, multiplicity]
    rows = [np.broadcast_to(row, (GRID, SPREAD)).reshape(DEVICES, 1, 2 * SPREAD) for row in rows]
    return jnp.asarray(np.concatenate(rows, axis=1), F32)


def chunk_of(k, slot):
    before = sum(len(chunks) for chunks in CHUNKS[:k])
    return before + next(i for i, (_, end) in enumerate(CHUNKS[k]) if slot < end)


def tile(index):
    return pl.ds(pl.multiple_of(index * 8, 8), 8)


def body(
    samples_hbm,
    packed_hbm,
    twist_hbm,
    beta_hbm,
    order_hbm,
    coef_ref,
    shares,
    samples,
    packed,
    twist,
    beta,
    order,
    spectrum,
    received,
    wigner,
    total,
    rows_of_level,
    placed,
    load_sem,
    send_sem,
    recv_sem,
):
    me = lax.axis_index("beta")
    place = (me // 16, me // 4 % 4, me % 4)

    def target(offset):
        z, y, x = ((place[axis] + offset[axis]) % 4 for axis in range(3))
        return z * 16 + y * 4 + x

    loads = [
        pltpu.make_async_copy(packed_hbm, packed, load_sem.at[0]),
        pltpu.make_async_copy(samples_hbm.at[0], samples.at[0], load_sem.at[1]),
        pltpu.make_async_copy(twist_hbm, twist, load_sem.at[2]),
        pltpu.make_async_copy(samples_hbm.at[1], samples.at[1], load_sem.at[3]),
        pltpu.make_async_copy(beta_hbm, beta, load_sem.at[4]),
        pltpu.make_async_copy(order_hbm.at[me], order, load_sem.at[5]),
    ]
    for load in loads:
        load.start()

    barrier = pltpu.get_barrier_semaphore()
    with jax.named_scope("greet"):
        for offset in OFFSETS:
            pl.semaphore_signal(
                barrier, 1, device_id={"beta": target(offset)}, device_id_type=MESH
            )

    def product(left, right):
        return jnp.dot(left, right, preferred_element_type=F32)

    def split(values):
        high = values.astype(BF16)
        return high, (values - high.astype(F32)).astype(BF16)

    def transform(k):
        high, low = split(samples[k].reshape(FUNCTIONS * GRID, GRID))
        halfway = product(jnp.concatenate([high, low], axis=1), packed[0:256, :])
        halfway = halfway + product(high, packed[256:384, :])
        twist_cos, twist_sin = twist[0:128, :], twist[128:256, :]
        alpha_high, alpha_low = packed[384:512, :], packed[512:640, :]
        for pair in range(2):
            turned = []
            for f in (2 * pair, 2 * pair + 1):
                part = halfway[f * GRID : (f + 1) * GRID]
                re, im = part[:, :128], part[:, 128:]
                turned.append(
                    jnp.concatenate(
                        [twist_cos * re + twist_sin * im, twist_cos * im - twist_sin * re], axis=0
                    )
                )
            turned_high, turned_low = split(jnp.concatenate(turned, axis=1))
            rows = (
                product(alpha_high, turned_high)
                + product(alpha_low, turned_high)
                + product(alpha_high, turned_low)
            )
            for s in range(2):
                for f in range(2):
                    spectrum[
                        pl.ds(k * HALF + s * FUNCTIONS + 2 * pair + f, DEVICES, stride=8), :
                    ] = rows[s * DEVICES : (s + 1) * DEVICES, f * 128 : (f + 1) * 128]

    def send(k):
        for slot, offset in enumerate(OFFSETS):
            other = target(offset)
            pltpu.make_async_remote_copy(
                src_ref=spectrum.at[tile(k * DEVICES + other), :],
                dst_ref=received.at[pl.ds(k * HALF + slot * 8, 8), :],
                send_sem=send_sem.at[0],
                recv_sem=recv_sem.at[chunk_of(k, slot)],
                device_id={"beta": other},
                device_id_type=MESH,
            ).start()

    with jax.named_scope("load0"):
        for load in loads[:3]:
            load.wait()
    with jax.named_scope("dft0"):
        transform(0)
    with jax.named_scope("load1"):
        for load in loads[3:]:
            load.wait()
    with jax.named_scope("dft1"):
        transform(1)
    with jax.named_scope("barrier_wait"):
        pl.semaphore_wait(barrier, OTHERS)
    with jax.named_scope("send"):
        send(0)
        send(1)
    for k in range(2):
        received[k * HALF + OTHERS * 8 : (k + 1) * HALF, :] = spectrum[tile(k * DEVICES + me), :]

    with jax.named_scope("coeff"):
        alpha_order, gamma_order = order[5:6, :], order[6:7, :]
        lowest = order[4:5, :]
        degree = lax.broadcasted_iota(jnp.int32, (SPREAD, 128), 0).astype(F32)
        previous = degree - 1.0
        upper = (degree * degree - alpha_order * alpha_order) * (
            degree * degree - gamma_order * gamma_order
        )
        lower = (previous * previous - alpha_order * alpha_order) * (
            previous * previous - gamma_order * gamma_order
        )
        root_upper = jnp.sqrt(jnp.maximum(upper, 1.0))
        rows_of_level[0] = degree * (2.0 * previous + 1.0) / root_upper
        rows_of_level[1] = alpha_order * gamma_order / jnp.maximum(previous * degree, 1.0)
        rows_of_level[2] = (
            degree * jnp.sqrt(jnp.maximum(lower, 0.0)) / (jnp.maximum(previous, 1.0) * root_upper)
        )
        beta[128:256, :] = (
            beta[384:512, :]
            * order[1:2, :]
            * jnp.exp(
                order[0:1, :] + order[2:3, :] * beta[128:256, :] + order[3:4, :] * beta[256:384, :]
            )
        )

    with jax.named_scope("arrange"):
        for slot, offset in enumerate(OFFSETS + [(0, 0, 0)]):
            sender = target(tuple((4 - step) % 4 for step in offset))
            for k in range(2):
                for table in range(2):
                    placed[table, k * DEVICES + slot : k * DEVICES + slot + 1, :] = beta[
                        pl.ds(sender + table * GRID + k * DEVICES, 1), :
                    ]

    with jax.named_scope("wigner"):
        for k in range(2):

            def advance(level, carried):
                former, current = carried
                f_row = rows_of_level[0, pl.ds(level, 1), :]
                c_row = rows_of_level[1, pl.ds(level, 1), :]
                b_row = rows_of_level[2, pl.ds(level, 1), :]
                starts = lowest == level.astype(F32)
                cosine = placed[0, k * DEVICES : (k + 1) * DEVICES, :]
                first = placed[1, k * DEVICES : (k + 1) * DEVICES, :]
                recurred = f_row * (cosine - c_row) * current - b_row * former
                renewed = jnp.where(starts, first, recurred)
                wigner[pl.ds(pl.multiple_of(level * GRID + k * DEVICES, 64), DEVICES), :] = renewed
                return current, renewed

            empty = placed[0, 0:DEVICES, :] * 0.0
            lax.fori_loop(0, SPREAD, advance, (empty, empty))

    def contract(k, begin, end, fresh):
        def level_block(block, _):
            rows = [pl.ds(pl.multiple_of(block * 128 + t * 8, 8), 8) for t in range(16)]
            if fresh:
                sums = tuple(rows_of_level[0, 0:8, :] * 0.0 for _ in range(16))
            else:
                sums = tuple(total[rows[t], :] for t in range(16))

            def gather(group, sums):
                sums = list(sums)
                base = group * 16
                for index in range(16):
                    values = received[
                        pl.ds(pl.multiple_of(base * 8, 8) + (k * DEVICES + begin + index) * 8, 8), :
                    ]
                    for t in range(16):
                        factor = wigner[
                            pl.ds(
                                block * 16 * GRID + base + (t * GRID + k * DEVICES + begin + index),
                                8,
                                stride=0,
                            ),
                            :,
                        ]
                        sums[t] = sums[t] + values * factor
                return tuple(sums)

            sums = lax.fori_loop(0, (end - begin) // 16, gather, sums)
            for t in range(16):
                total[rows[t], :] = sums[t]
            return 0

        lax.fori_loop(0, 4, level_block, 0)

    for k in range(2):
        for begin, end in CHUNKS[k][::-1]:
            count = min(end, OTHERS) - begin
            with jax.named_scope(f"wait{k}_{begin}"):
                pltpu.make_async_remote_copy(
                    src_ref=spectrum.at[0 : count * 8, :],
                    dst_ref=received.at[0 : count * 8, :],
                    send_sem=send_sem.at[0],
                    recv_sem=recv_sem.at[chunk_of(k, begin)],
                    device_id={"beta": target(OFFSETS[0])},
                    device_id_type=MESH,
                ).wait_recv()
            with jax.named_scope(f"contract{k}_{begin}"):
                contract(k, begin, end, k == 0 and begin == 0)

    with jax.named_scope("finish"):
        scale = 8.0 * jnp.sqrt(2.0 * degree + 1.0)
        coeffs = []
        for channel in range(CHANNELS):
            coeffs.append(total[pl.ds(channel, SPREAD, stride=CHANNELS), :] * scale)
        squares = jnp.concatenate(
            [coeffs[f] * coeffs[f] + coeffs[f + 4] * coeffs[f + 4] for f in range(FUNCTIONS)], axis=0
        )
        squares_high, squares_low = split(squares)
        multiplicity = jnp.broadcast_to(order[7:8, :], (16, 128)).astype(BF16)

        def lane_sum(values):
            return lax.dot_general(
                multiplicity, values, (((1,), (1,)), ((), ())), preferred_element_type=F32
            )

        energy = lane_sum(squares_high) + lane_sum(squares_low)
        lane = lax.broadcasted_iota(jnp.int32, (1, 128), 1)
        degrees = 2.0 * (lane % SPREAD).astype(F32) + 1.0
        inverse = 1.0 / (degrees * degrees)
        shares[me, 0:1, :] = energy[0:1, :128] * inverse
        shares[me, 1:2, :] = energy[0:1, 128:] * inverse

    with jax.named_scope("share_send"):
        for offset in OFFSETS:
            pltpu.make_async_remote_copy(
                src_ref=shares.at[me],
                dst_ref=shares.at[me],
                send_sem=send_sem.at[1],
                recv_sem=recv_sem.at[chunk_of(2, 0)],
                device_id={"beta": target(offset)},
                device_id_type=MESH,
            ).start()

    with jax.named_scope("store"):
        for channel in range(CHANNELS):
            coef_ref[0, channel] = coeffs[channel][:, :SPREAD]
            coef_ref[1, channel] = coeffs[channel][:, SPREAD:]

    with jax.named_scope("sent"):
        for k in range(2):
            pltpu.make_async_remote_copy(
                src_ref=spectrum.at[0 : OTHERS * 8, :],
                dst_ref=received.at[0 : OTHERS * 8, :],
                send_sem=send_sem.at[0],
                recv_sem=recv_sem.at[0],
                device_id={"beta": target(OFFSETS[0])},
                device_id_type=MESH,
            ).wait_send()

    with jax.named_scope("share_wait"):
        shared = pltpu.make_async_remote_copy(
            src_ref=shares.at[0:OTHERS],
            dst_ref=shares.at[0:OTHERS],
            send_sem=send_sem.at[1],
            recv_sem=recv_sem.at[chunk_of(2, 0)],
            device_id={"beta": target(OFFSETS[0])},
            device_id_type=MESH,
        )
        shared.wait_send()
        shared.wait_recv()


def tail(coef_ref, shares, coef_hbm, power_hbm, power, sem):
    store = pltpu.make_async_copy(coef_ref, coef_hbm, sem.at[0])
    store.start()
    sums = [shares[index] for index in range(4)]
    for index in range(4, DEVICES):
        sums[index % 4] = sums[index % 4] + shares[index]
    result = (sums[0] + sums[1]) + (sums[2] + sums[3])
    for f in range(FUNCTIONS):
        power[f : f + 1, :] = result[f // 2 : f // 2 + 1, f % 2 * 64 : f % 2 * 64 + 64]
    finish = pltpu.make_async_copy(power, power_hbm, sem.at[1])
    finish.start()
    store.wait()
    finish.wait()


def local(samples):
    packed, twist = fourier_tables()
    anywhere = pl.BlockSpec(memory_space=pl.ANY)
    vmem = pl.BlockSpec(memory_space=pltpu.VMEM)
    coef, shares = pl.pallas_call(
        body,
        out_shape=(
            pltpu.VMEM((2, CHANNELS, SPREAD, SPREAD), F32),
            pltpu.VMEM((DEVICES, 2, 128), F32),
        ),
        in_specs=[anywhere] * 5,
        out_specs=(vmem, vmem),
        scratch_shapes=[
            pltpu.VMEM((2, FUNCTIONS, GRID, GRID), F32),
            pltpu.VMEM((640, 256), BF16),
            pltpu.VMEM((256, 128), F32),
            pltpu.VMEM((512, 128), F32),
            pltpu.VMEM((8, 128), F32),
            pltpu.VMEM((2 * HALF, 128), F32),
            pltpu.VMEM((2 * HALF, 128), F32),
            pltpu.VMEM((SPREAD * GRID, 128), F32),
            pltpu.VMEM((SPREAD * CHANNELS, 128), F32),
            pltpu.VMEM((3, SPREAD, 128), F32),
            pltpu.VMEM((2, GRID, 128), F32),
            pltpu.SemaphoreType.DMA((6,)),
            pltpu.SemaphoreType.DMA((2,)),
            pltpu.SemaphoreType.DMA((sum(map(len, CHUNKS)),)),
        ],
        compiler_params=pltpu.CompilerParams(collective_id=0, has_side_effects=True),
        name="rotation_transform",
    )(samples, packed, twist, beta_tables(), order_tables())
    coef, power = pl.pallas_call(
        tail,
        out_shape=(
            jax.ShapeDtypeStruct((2, CHANNELS, SPREAD, SPREAD), F32),
            jax.ShapeDtypeStruct((FUNCTIONS, SPREAD), F32),
        ),
        in_specs=[vmem, vmem],
        out_specs=(anywhere, anywhere),
        scratch_shapes=[pltpu.VMEM((FUNCTIONS, SPREAD), F32), pltpu.SemaphoreType.DMA((2,))],
        compiler_params=pltpu.CompilerParams(vmem_limit_bytes=4 * 1024 * 1024),
        name="store_results",
    )(coef, shares)
    return coef.reshape(2, 2, FUNCTIONS, SPREAD, SPREAD), power


def solution(mesh):
    return jax.shard_map(
        local,
        mesh=mesh,
        in_specs=(P("beta", "grp", None, None),),
        out_specs=(P("beta", None, "grp", None, None), P("grp", None)),
        check_vma=False,
    )
```

```python
import itertools
import math

import jax
import jax.numpy as jnp
import numpy as np
from jax import lax
from jax.experimental import pallas as pl
from jax.experimental.pallas import tpu as pltpu
from jax.sharding import PartitionSpec as P

MESH = pl.DeviceIdType.MESH
F32 = jnp.float32
BF16 = jnp.bfloat16

GRID = 128
SPREAD = 64
FUNCTIONS = 4
CHANNELS = 8
DEVICES = 64
OTHERS = DEVICES - 1
HALF = DEVICES * CHANNELS
SEND_COST = (0.0, 1.0, 2.2, 1.65)
GREET_COST = (0.0, 1.65, 2.2, 1.0)


def far_first(cost):
    near = [o for o in itertools.product(range(4), repeat=3) if o != (0, 0, 0)]
    order = []
    for z, y, x in near:
        for turn in ((z, y, x), (y, x, z), (x, z, y)):
            for offset in (turn, tuple((4 - step) % 4 for step in turn)):
                if offset not in order:
                    order.append(offset)
    return sorted(order, key=lambda o: -sum(cost[step] for step in o))


OFFSETS = far_first(SEND_COST)
GREETINGS = far_first(GREET_COST)
CHUNKS = (((0, 64),), ((0, 32), (32, 48), (48, 64)), ((0, 64),))


def split_bf16(table):
    high = jnp.asarray(table, F32).astype(BF16)
    low = (jnp.asarray(table, F32) - high.astype(F32)).astype(BF16)
    return high, low


def fourier_tables():
    g = np.arange(GRID)
    q = np.arange(SPREAD)
    gamma = 2.0 * np.pi * ((g[:, None] * q[None, :]) % GRID) / GRID
    cosine, minus_sine = np.cos(gamma), -np.sin(gamma)
    first = np.concatenate([cosine, cosine, minus_sine, minus_sine], axis=1)
    j = np.arange(DEVICES)
    alpha = 2.0 * np.pi * ((2 * j[:, None] * g[None, :]) % GRID) / GRID
    c, s = np.cos(alpha) / GRID, np.sin(alpha) / GRID
    second = np.concatenate(
        [np.concatenate([c, s], axis=1), np.concatenate([-s, c], axis=1)], axis=0
    )
    first_high, first_low = split_bf16(first)
    packed = jnp.concatenate([first_high, first_high, first_low, *split_bf16(second)], axis=0)
    turn = 2.0 * np.pi * g / GRID
    ones = np.ones((GRID, SPREAD))
    twist_cos = np.concatenate([ones, np.cos(turn)[:, None] * ones], axis=1)
    twist_sin = np.concatenate([0.0 * ones, np.sin(turn)[:, None] * ones], axis=1)
    return packed, jnp.asarray(np.concatenate([twist_cos, twist_sin], axis=0), F32)


def beta_tables():
    k = np.arange(GRID).reshape(DEVICES, 2).T.reshape(GRID)
    angles = np.pi * (2 * k + 1) / 256.0
    odd = 2.0 * np.arange(SPREAD) + 1.0
    weight = (2.0 / SPREAD) * np.sin(angles)
    weight = weight * np.sum(np.sin(angles[:, None] * odd) / odd, axis=1)
    columns = [np.cos(angles), np.log(np.cos(angles / 2)), np.log(np.sin(angles / 2)), weight]
    tables = [np.repeat(column[:, None], GRID, axis=1) for column in columns]
    return jnp.asarray(np.concatenate(tables, axis=0), F32)


def order_tables():
    lgamma = np.array([math.lgamma(v + 1.0) for v in range(2 * GRID + 1)])
    n = np.arange(GRID)
    p = np.where(n < SPREAD, n, n - GRID)[:, None]
    q = np.arange(SPREAD)[None, :]
    lowest = np.maximum(np.abs(p), q)
    t = np.maximum(0, q - p)
    magnitude = 0.5 * (
        lgamma[lowest + p] + lgamma[lowest - p] + lgamma[lowest + q] + lgamma[lowest - q]
    )
    magnitude = magnitude - lgamma[lowest + q - t] - lgamma[t]
    magnitude = magnitude - lgamma[p - q + t] - lgamma[lowest - p - t]
    sign = 1.0 - 2.0 * ((p - q + t) % 2)
    cos_power = 2 * lowest + q - p - 2 * t
    sin_power = p - q + 2 * t
    multiplicity = np.where(q == 0, 1.0, 2.0)
    rows = [magnitude, sign, cos_power, sin_power, lowest, p, q, multiplicity]
    rows = [np.broadcast_to(row, (GRID, SPREAD)).reshape(DEVICES, 1, 2 * SPREAD) for row in rows]
    return jnp.asarray(np.concatenate(rows, axis=1), F32)


def chunk_of(k, slot):
    before = sum(len(chunks) for chunks in CHUNKS[:k])
    return before + next(i for i, (_, end) in enumerate(CHUNKS[k]) if slot < end)


def tile(index):
    return pl.ds(pl.multiple_of(index * 8, 8), 8)


def body(
    samples_hbm,
    packed_hbm,
    twist_hbm,
    beta_hbm,
    order_hbm,
    coef_ref,
    shares,
    samples,
    packed,
    twist,
    beta,
    order,
    spectrum,
    received,
    wigner,
    total,
    rows_of_level,
    placed,
    load_sem,
    send_sem,
    recv_sem,
):
    me = lax.axis_index("beta")
    place = (me // 16, me // 4 % 4, me % 4)

    def target(offset):
        z, y, x = ((place[axis] + offset[axis]) % 4 for axis in range(3))
        return z * 16 + y * 4 + x

    loads = [
        pltpu.make_async_copy(packed_hbm, packed, load_sem.at[0]),
        pltpu.make_async_copy(samples_hbm.at[0], samples.at[0], load_sem.at[1]),
        pltpu.make_async_copy(twist_hbm, twist, load_sem.at[2]),
        pltpu.make_async_copy(samples_hbm.at[1], samples.at[1], load_sem.at[3]),
        pltpu.make_async_copy(beta_hbm, beta, load_sem.at[4]),
        pltpu.make_async_copy(order_hbm.at[me], order, load_sem.at[5]),
    ]
    for load in loads:
        load.start()

    barrier = pltpu.get_barrier_semaphore()
    with jax.named_scope("greet"):
        for offset in GREETINGS:
            pl.semaphore_signal(
                barrier, 1, device_id={"beta": target(offset)}, device_id_type=MESH
            )

    def product(left, right):
        return jnp.dot(left, right, preferred_element_type=F32)

    def split(values):
        high = values.astype(BF16)
        return high, (values - high.astype(F32)).astype(BF16)

    def transform(k):
        high, low = split(samples[k].reshape(FUNCTIONS * GRID, GRID))
        halfway = product(jnp.concatenate([high, low], axis=1), packed[0:256, :])
        halfway = halfway + product(high, packed[256:384, :])
        twist_cos, twist_sin = twist[0:128, :], twist[128:256, :]
        alpha_high, alpha_low = packed[384:512, :], packed[512:640, :]
        for pair in range(2):
            turned = []
            for f in (2 * pair, 2 * pair + 1):
                part = halfway[f * GRID : (f + 1) * GRID]
                re, im = part[:, :128], part[:, 128:]
                turned.append(
                    jnp.concatenate(
                        [twist_cos * re + twist_sin * im, twist_cos * im - twist_sin * re], axis=0
                    )
                )
            turned_high, turned_low = split(jnp.concatenate(turned, axis=1))
            rows = (
                product(alpha_high, turned_high)
                + product(alpha_low, turned_high)
                + product(alpha_high, turned_low)
            )
            for s in range(2):
                for f in range(2):
                    spectrum[
                        pl.ds(k * HALF + s * FUNCTIONS + 2 * pair + f, DEVICES, stride=8), :
                    ] = rows[s * DEVICES : (s + 1) * DEVICES, f * 128 : (f + 1) * 128]

    def send(k):
        for slot, offset in enumerate(OFFSETS):
            other = target(offset)
            pltpu.make_async_remote_copy(
                src_ref=spectrum.at[tile(k * DEVICES + other), :],
                dst_ref=received.at[pl.ds(k * HALF + slot * 8, 8), :],
                send_sem=send_sem.at[0],
                recv_sem=recv_sem.at[chunk_of(k, slot)],
                device_id={"beta": other},
                device_id_type=MESH,
            ).start()

    with jax.named_scope("load0"):
        for load in loads[:3]:
            load.wait()
    with jax.named_scope("dft0"):
        transform(0)
    with jax.named_scope("load1"):
        for load in loads[3:]:
            load.wait()
    with jax.named_scope("dft1"):
        transform(1)
    with jax.named_scope("barrier_wait"):
        pl.semaphore_wait(barrier, OTHERS)
    with jax.named_scope("send"):
        send(0)

        @pl.when(lax.axis_index("grp") == 0)
        def _():
            send(1)
    for k in range(2):
        received[k * HALF + OTHERS * 8 : (k + 1) * HALF, :] = spectrum[tile(k * DEVICES + me), :]

    with jax.named_scope("coeff"):
        alpha_order, gamma_order = order[5:6, :], order[6:7, :]
        lowest = order[4:5, :]
        degree = lax.broadcasted_iota(jnp.int32, (SPREAD, 128), 0).astype(F32)
        previous = degree - 1.0
        upper = (degree * degree - alpha_order * alpha_order) * (
            degree * degree - gamma_order * gamma_order
        )
        lower = (previous * previous - alpha_order * alpha_order) * (
            previous * previous - gamma_order * gamma_order
        )
        root_upper = jnp.sqrt(jnp.maximum(upper, 1.0))
        rows_of_level[0] = degree * (2.0 * previous + 1.0) / root_upper
        rows_of_level[1] = alpha_order * gamma_order / jnp.maximum(previous * degree, 1.0)
        rows_of_level[2] = (
            degree * jnp.sqrt(jnp.maximum(lower, 0.0)) / (jnp.maximum(previous, 1.0) * root_upper)
        )
        beta[128:256, :] = (
            beta[384:512, :]
            * order[1:2, :]
            * jnp.exp(
                order[0:1, :] + order[2:3, :] * beta[128:256, :] + order[3:4, :] * beta[256:384, :]
            )
        )

    with jax.named_scope("arrange"):
        for slot, offset in enumerate(OFFSETS + [(0, 0, 0)]):
            sender = target(tuple((4 - step) % 4 for step in offset))
            for k in range(2):
                for table in range(2):
                    placed[table, k * DEVICES + slot : k * DEVICES + slot + 1, :] = beta[
                        pl.ds(sender + table * GRID + k * DEVICES, 1), :
                    ]

    with jax.named_scope("wigner"):
        for k in range(2):

            def advance(level, carried):
                former, current = carried
                f_row = rows_of_level[0, pl.ds(level, 1), :]
                c_row = rows_of_level[1, pl.ds(level, 1), :]
                b_row = rows_of_level[2, pl.ds(level, 1), :]
                starts = lowest == level.astype(F32)
                cosine = placed[0, k * DEVICES : (k + 1) * DEVICES, :]
                first = placed[1, k * DEVICES : (k + 1) * DEVICES, :]
                recurred = f_row * (cosine - c_row) * current - b_row * former
                renewed = jnp.where(starts, first, recurred)
                wigner[pl.ds(pl.multiple_of(level * GRID + k * DEVICES, 64), DEVICES), :] = renewed
                return current, renewed

            empty = placed[0, 0:DEVICES, :] * 0.0
            lax.fori_loop(0, SPREAD, advance, (empty, empty))

    with jax.named_scope("send_late"):

        @pl.when(lax.axis_index("grp") == 1)
        def _():
            send(1)

    smallest = jnp.minimum(2 * me, 2 * DEVICES - 1 - 2 * me)
    first_block = smallest // 16
    total[...] = jnp.zeros((SPREAD * CHANNELS, 128), F32)

    def contract(k, begin, end):
        def level_block(block, _):
            rows = [pl.ds(pl.multiple_of(block * 128 + t * 8, 8), 8) for t in range(16)]
            sums = tuple(total[rows[t], :] for t in range(16))

            def gather(group, sums):
                sums = list(sums)
                base = group * 16
                for index in range(16):
                    values = received[
                        pl.ds(pl.multiple_of(base * 8, 8) + (k * DEVICES + begin + index) * 8, 8), :
                    ]
                    for t in range(16):
                        factor = wigner[
                            pl.ds(
                                block * 16 * GRID + base + (t * GRID + k * DEVICES + begin + index),
                                8,
                                stride=0,
                            ),
                            :,
                        ]
                        sums[t] = sums[t] + values * factor
                return tuple(sums)

            sums = lax.fori_loop(0, (end - begin) // 16, gather, sums)
            for t in range(16):
                total[rows[t], :] = sums[t]
            return 0

        lax.fori_loop(first_block, 4, level_block, 0)

    for k in range(2):
        for begin, end in CHUNKS[k][::-1]:
            count = min(end, OTHERS) - begin
            with jax.named_scope(f"wait{k}_{begin}"):
                pltpu.make_async_remote_copy(
                    src_ref=spectrum.at[0 : count * 8, :],
                    dst_ref=received.at[0 : count * 8, :],
                    send_sem=send_sem.at[0],
                    recv_sem=recv_sem.at[chunk_of(k, begin)],
                    device_id={"beta": target(OFFSETS[0])},
                    device_id_type=MESH,
                ).wait_recv()
            with jax.named_scope(f"contract{k}_{begin}"):
                contract(k, begin, end)

    with jax.named_scope("finish"):
        scale = 8.0 * jnp.sqrt(2.0 * degree + 1.0)
        coeffs = []
        for channel in range(CHANNELS):
            coeffs.append(total[pl.ds(channel, SPREAD, stride=CHANNELS), :] * scale)
        squares = jnp.concatenate(
            [coeffs[f] * coeffs[f] + coeffs[f + 4] * coeffs[f + 4] for f in range(FUNCTIONS)], axis=0
        )
        squares_high, squares_low = split(squares)
        multiplicity = jnp.broadcast_to(order[7:8, :], (16, 128)).astype(BF16)

        def lane_sum(values):
            return lax.dot_general(
                multiplicity, values, (((1,), (1,)), ((), ())), preferred_element_type=F32
            )

        energy = lane_sum(squares_high) + lane_sum(squares_low)
        lane = lax.broadcasted_iota(jnp.int32, (1, 128), 1)
        degrees = 2.0 * (lane % SPREAD).astype(F32) + 1.0
        inverse = 1.0 / (degrees * degrees)
        shares[me, 0:1, :] = energy[0:1, :128] * inverse
        shares[me, 1:2, :] = energy[0:1, 128:] * inverse

    with jax.named_scope("share_send"):
        for offset in OFFSETS:
            pltpu.make_async_remote_copy(
                src_ref=shares.at[me],
                dst_ref=shares.at[me],
                send_sem=send_sem.at[1],
                recv_sem=recv_sem.at[chunk_of(2, 0)],
                device_id={"beta": target(offset)},
                device_id_type=MESH,
            ).start()

    with jax.named_scope("store"):
        for channel in range(CHANNELS):
            coef_ref[0, channel] = coeffs[channel][:, :SPREAD]
            coef_ref[1, channel] = coeffs[channel][:, SPREAD:]

    with jax.named_scope("sent"):
        for k in range(2):
            pltpu.make_async_remote_copy(
                src_ref=spectrum.at[0 : OTHERS * 8, :],
                dst_ref=received.at[0 : OTHERS * 8, :],
                send_sem=send_sem.at[0],
                recv_sem=recv_sem.at[0],
                device_id={"beta": target(OFFSETS[0])},
                device_id_type=MESH,
            ).wait_send()

    with jax.named_scope("share_wait"):
        shared = pltpu.make_async_remote_copy(
            src_ref=shares.at[0:OTHERS],
            dst_ref=shares.at[0:OTHERS],
            send_sem=send_sem.at[1],
            recv_sem=recv_sem.at[chunk_of(2, 0)],
            device_id={"beta": target(OFFSETS[0])},
            device_id_type=MESH,
        )
        shared.wait_send()
        shared.wait_recv()


def tail(coef_ref, shares, coef_hbm, power_hbm, power, sem):
    store = pltpu.make_async_copy(coef_ref, coef_hbm, sem.at[0])
    store.start()
    sums = [shares[index] for index in range(4)]
    for index in range(4, DEVICES):
        sums[index % 4] = sums[index % 4] + shares[index]
    result = (sums[0] + sums[1]) + (sums[2] + sums[3])
    for f in range(FUNCTIONS):
        power[f : f + 1, :] = result[f // 2 : f // 2 + 1, f % 2 * 64 : f % 2 * 64 + 64]
    finish = pltpu.make_async_copy(power, power_hbm, sem.at[1])
    finish.start()
    store.wait()
    finish.wait()


def local(samples):
    packed, twist = fourier_tables()
    anywhere = pl.BlockSpec(memory_space=pl.ANY)
    vmem = pl.BlockSpec(memory_space=pltpu.VMEM)
    coef, shares = pl.pallas_call(
        body,
        out_shape=(
            pltpu.VMEM((2, CHANNELS, SPREAD, SPREAD), F32),
            pltpu.VMEM((DEVICES, 2, 128), F32),
        ),
        in_specs=[anywhere] * 5,
        out_specs=(vmem, vmem),
        scratch_shapes=[
            pltpu.VMEM((2, FUNCTIONS, GRID, GRID), F32),
            pltpu.VMEM((640, 256), BF16),
            pltpu.VMEM((256, 128), F32),
            pltpu.VMEM((512, 128), F32),
            pltpu.VMEM((8, 128), F32),
            pltpu.VMEM((2 * HALF, 128), F32),
            pltpu.VMEM((2 * HALF, 128), F32),
            pltpu.VMEM((SPREAD * GRID, 128), F32),
            pltpu.VMEM((SPREAD * CHANNELS, 128), F32),
            pltpu.VMEM((3, SPREAD, 128), F32),
            pltpu.VMEM((2, GRID, 128), F32),
            pltpu.SemaphoreType.DMA((6,)),
            pltpu.SemaphoreType.DMA((2,)),
            pltpu.SemaphoreType.DMA((sum(map(len, CHUNKS)),)),
        ],
        compiler_params=pltpu.CompilerParams(collective_id=0, has_side_effects=True),
        name="rotation_transform",
    )(samples, packed, twist, beta_tables(), order_tables())
    coef, power = pl.pallas_call(
        tail,
        out_shape=(
            jax.ShapeDtypeStruct((2, CHANNELS, SPREAD, SPREAD), F32),
            jax.ShapeDtypeStruct((FUNCTIONS, SPREAD), F32),
        ),
        in_specs=[vmem, vmem],
        out_specs=(anywhere, anywhere),
        scratch_shapes=[pltpu.VMEM((FUNCTIONS, SPREAD), F32), pltpu.SemaphoreType.DMA((2,))],
        compiler_params=pltpu.CompilerParams(vmem_limit_bytes=4 * 1024 * 1024),
        name="store_results",
    )(coef, shares)
    return coef.reshape(2, 2, FUNCTIONS, SPREAD, SPREAD), power


def solution(mesh):
    return jax.shard_map(
        local,
        mesh=mesh,
        in_specs=(P("beta", "grp", None, None),),
        out_specs=(P("beta", None, "grp", None, None), P("grp", None)),
        check_vma=False,
    )
```

```python
import itertools
import math

import jax
import jax.numpy as jnp
import numpy as np
from jax import lax
from jax.experimental import pallas as pl
from jax.experimental.pallas import tpu as pltpu
from jax.sharding import PartitionSpec as P

MESH = pl.DeviceIdType.MESH
F32 = jnp.float32
BF16 = jnp.bfloat16

GRID = 128
SPREAD = 64
FUNCTIONS = 4
CHANNELS = 8
DEVICES = 64
OTHERS = DEVICES - 1
HALF = DEVICES * CHANNELS
LOW = SPREAD // 2
PACKED = 48
SEND_COST = (0.0, 1.0, 2.2, 1.65)
GREET_COST = (0.0, 1.65, 2.2, 1.0)


def far_first(cost):
    near = [o for o in itertools.product(range(4), repeat=3) if o != (0, 0, 0)]
    order = []
    for z, y, x in near:
        for turn in ((z, y, x), (y, x, z), (x, z, y)):
            for offset in (turn, tuple((4 - step) % 4 for step in turn)):
                if offset not in order:
                    order.append(offset)
    return sorted(order, key=lambda o: -sum(cost[step] for step in o))


OFFSETS = far_first(SEND_COST)
GREETINGS = far_first(GREET_COST)
CHUNKS = (((0, 16), (16, 32), (32, 64)), ((0, 16), (16, 32), (32, 48), (48, 64)), ((0, 64),))


def lanes(even, odd):
    return np.concatenate(
        [even[..., :LOW], odd[..., :LOW], even[..., LOW:], odd[..., LOW:]], axis=-1
    )


def split_bf16(table):
    high = jnp.asarray(table, F32).astype(BF16)
    low = (jnp.asarray(table, F32) - high.astype(F32)).astype(BF16)
    return high, low


def fourier_tables():
    g = np.arange(GRID)
    q = np.arange(SPREAD)
    gamma = 2.0 * np.pi * ((g[:, None] * q[None, :]) % GRID) / GRID
    cosine, minus_sine = np.cos(gamma), -np.sin(gamma)
    first = np.concatenate(
        [lanes(cosine, cosine), lanes(minus_sine, minus_sine)], axis=1
    )
    j = np.arange(DEVICES)
    alpha = 2.0 * np.pi * ((2 * j[:, None] * g[None, :]) % GRID) / GRID
    c, s = np.cos(alpha) / GRID, np.sin(alpha) / GRID
    second = np.concatenate(
        [np.concatenate([c, s], axis=1), np.concatenate([-s, c], axis=1)], axis=0
    )
    first_high, first_low = split_bf16(first)
    packed = jnp.concatenate([first_high, first_high, first_low, *split_bf16(second)], axis=0)
    turn = 2.0 * np.pi * g / GRID
    ones = np.ones((GRID, SPREAD))
    twist_cos = lanes(ones, np.cos(turn)[:, None] * ones)
    twist_sin = lanes(0.0 * ones, np.sin(turn)[:, None] * ones)
    return packed, jnp.asarray(np.concatenate([twist_cos, twist_sin], axis=0), F32)


def beta_tables():
    k = np.arange(GRID).reshape(DEVICES, 2).T.reshape(GRID)
    angles = np.pi * (2 * k + 1) / 256.0
    odd = 2.0 * np.arange(SPREAD) + 1.0
    weight = (2.0 / SPREAD) * np.sin(angles)
    weight = weight * np.sum(np.sin(angles[:, None] * odd) / odd, axis=1)
    columns = [np.cos(angles), np.log(np.cos(angles / 2)), np.log(np.sin(angles / 2)), weight]
    tables = [np.repeat(column[:, None], GRID, axis=1) for column in columns]
    return jnp.asarray(np.concatenate(tables, axis=0), F32)


def order_tables():
    lgamma = np.array([math.lgamma(v + 1.0) for v in range(2 * GRID + 1)])
    n = np.arange(GRID)
    p = np.where(n < SPREAD, n, n - GRID)[:, None]
    q = np.arange(SPREAD)[None, :]
    lowest = np.maximum(np.abs(p), q)
    t = np.maximum(0, q - p)
    magnitude = 0.5 * (
        lgamma[lowest + p] + lgamma[lowest - p] + lgamma[lowest + q] + lgamma[lowest - q]
    )
    magnitude = magnitude - lgamma[lowest + q - t] - lgamma[t]
    magnitude = magnitude - lgamma[p - q + t] - lgamma[lowest - p - t]
    sign = 1.0 - 2.0 * ((p - q + t) % 2)
    cos_power = 2 * lowest + q - p - 2 * t
    sin_power = p - q + 2 * t
    multiplicity = np.where(q == 0, 1.0, 2.0)
    rows = [magnitude, sign, cos_power, sin_power, lowest, p, q, multiplicity]
    rows = [np.broadcast_to(row, (GRID, SPREAD)).reshape(DEVICES, 2, SPREAD) for row in rows]
    return jnp.asarray(np.stack([lanes(row[:, 0], row[:, 1]) for row in rows], axis=1), F32)


def chunk_of(k, slot):
    before = sum(len(chunks) for chunks in CHUNKS[:k])
    return before + next(i for i, (_, end) in enumerate(CHUNKS[k]) if slot < end)


def tile(index):
    return pl.ds(pl.multiple_of(index * 8, 8), 8)


def body(
    samples_hbm,
    packed_hbm,
    twist_hbm,
    beta_hbm,
    order_hbm,
    coef_ref,
    shares,
    samples,
    packed,
    twist,
    beta,
    order,
    spectrum,
    received,
    wigner,
    total,
    rows_of_level,
    placed,
    load_sem,
    send_sem,
    recv_sem,
):
    me = lax.axis_index("beta")
    place = (me // 16, me // 4 % 4, me % 4)

    def target(offset):
        z, y, x = ((place[axis] + offset[axis]) % 4 for axis in range(3))
        return z * 16 + y * 4 + x

    loads = [
        pltpu.make_async_copy(packed_hbm, packed, load_sem.at[0]),
        pltpu.make_async_copy(samples_hbm.at[0], samples.at[0], load_sem.at[1]),
        pltpu.make_async_copy(twist_hbm, twist, load_sem.at[2]),
        pltpu.make_async_copy(samples_hbm.at[1], samples.at[1], load_sem.at[3]),
        pltpu.make_async_copy(beta_hbm, beta, load_sem.at[4]),
        pltpu.make_async_copy(order_hbm.at[me], order, load_sem.at[5]),
    ]
    for load in loads:
        load.start()

    barrier = pltpu.get_barrier_semaphore()
    with jax.named_scope("greet"):
        for offset in GREETINGS:
            pl.semaphore_signal(
                barrier, 1, device_id={"beta": target(offset)}, device_id_type=MESH
            )

    def product(left, right):
        return jnp.dot(left, right, preferred_element_type=F32)

    def split(values):
        high = values.astype(BF16)
        return high, (values - high.astype(F32)).astype(BF16)

    def transform(k):
        high, low = split(samples[k].reshape(FUNCTIONS * GRID, GRID))
        halfway = product(jnp.concatenate([high, low], axis=1), packed[0:256, :])
        halfway = halfway + product(high, packed[256:384, :])
        twist_cos, twist_sin = twist[0:128, :], twist[128:256, :]
        alpha_high, alpha_low = packed[384:512, :], packed[512:640, :]
        for pair in range(2):
            turned = []
            for f in (2 * pair, 2 * pair + 1):
                part = halfway[f * GRID : (f + 1) * GRID]
                re, im = part[:, :128], part[:, 128:]
                turned.append(
                    jnp.concatenate(
                        [twist_cos * re + twist_sin * im, twist_cos * im - twist_sin * re], axis=0
                    )
                )
            turned_high, turned_low = split(jnp.concatenate(turned, axis=1))
            rows = (
                product(alpha_high, turned_high)
                + product(alpha_low, turned_high)
                + product(alpha_high, turned_low)
            )
            for s in range(2):
                for f in range(2):
                    spectrum[
                        pl.ds(k * HALF + s * FUNCTIONS + 2 * pair + f, DEVICES, stride=8), :
                    ] = rows[s * DEVICES : (s + 1) * DEVICES, f * 128 : (f + 1) * 128]

    def send(k):
        for slot, offset in enumerate(OFFSETS):
            other = target(offset)
            pltpu.make_async_remote_copy(
                src_ref=spectrum.at[tile(k * DEVICES + other), :],
                dst_ref=received.at[pl.ds(k * HALF + slot * 8, 8), :],
                send_sem=send_sem.at[0],
                recv_sem=recv_sem.at[chunk_of(k, slot)],
                device_id={"beta": other},
                device_id_type=MESH,
            ).start()

    with jax.named_scope("load0"):
        for load in loads[:3]:
            load.wait()
    with jax.named_scope("dft0"):
        transform(0)
    with jax.named_scope("load1"):
        for load in loads[3:]:
            load.wait()
    with jax.named_scope("dft1"):
        transform(1)
    with jax.named_scope("barrier_wait"):
        pl.semaphore_wait(barrier, OTHERS)
    with jax.named_scope("send"):
        send(0)

        @pl.when(lax.axis_index("grp") == 0)
        def _():
            send(1)
    for k in range(2):
        received[k * HALF + OTHERS * 8 : (k + 1) * HALF, :] = spectrum[tile(k * DEVICES + me), :]

    with jax.named_scope("coeff"):
        alpha_order, gamma_order = order[5:6, :], order[6:7, :]
        lowest = order[4:5, :]
        degree = lax.broadcasted_iota(jnp.int32, (SPREAD, 128), 0).astype(F32)
        previous = degree - 1.0
        upper = (degree * degree - alpha_order * alpha_order) * (
            degree * degree - gamma_order * gamma_order
        )
        lower = (previous * previous - alpha_order * alpha_order) * (
            previous * previous - gamma_order * gamma_order
        )
        root_upper = jnp.sqrt(jnp.maximum(upper, 1.0))
        rows_of_level[0] = degree * (2.0 * previous + 1.0) / root_upper
        rows_of_level[1] = alpha_order * gamma_order / jnp.maximum(previous * degree, 1.0)
        rows_of_level[2] = (
            degree * jnp.sqrt(jnp.maximum(lower, 0.0)) / (jnp.maximum(previous, 1.0) * root_upper)
        )
        beta[128:256, :] = (
            beta[384:512, :]
            * order[1:2, :]
            * jnp.exp(
                order[0:1, :] + order[2:3, :] * beta[128:256, :] + order[3:4, :] * beta[256:384, :]
            )
        )

    with jax.named_scope("arrange"):
        for slot, offset in enumerate(OFFSETS + [(0, 0, 0)]):
            sender = target(tuple((4 - step) % 4 for step in offset))
            for k in range(2):
                for table in range(2):
                    placed[table, k * DEVICES + slot : k * DEVICES + slot + 1, :] = beta[
                        pl.ds(sender + table * GRID + k * DEVICES, 1), :
                    ]

    with jax.named_scope("wigner"):
        for k in range(2):

            def advance(level, carried):
                former, current = carried
                f_row = rows_of_level[0, pl.ds(level, 1), :]
                c_row = rows_of_level[1, pl.ds(level, 1), :]
                b_row = rows_of_level[2, pl.ds(level, 1), :]
                starts = lowest == level.astype(F32)
                cosine = placed[0, k * DEVICES : (k + 1) * DEVICES, :]
                first = placed[1, k * DEVICES : (k + 1) * DEVICES, :]
                recurred = f_row * (cosine - c_row) * current - b_row * former
                return current, jnp.where(starts, first, recurred)

            def where_to(row):
                return pl.ds(pl.multiple_of(row * GRID + k * DEVICES, 64), DEVICES)

            def lower(level, carried):
                carried = advance(level, carried)
                wigner[where_to(level), :] = carried[1]
                return carried

            def middle(level, carried):
                carried = advance(level, carried)
                moved = pltpu.roll(carried[1], 64, 1)
                wigner[where_to(level - 16), :] = wigner[where_to(level - 16), :] + moved
                return carried

            def upper(level, carried):
                carried = advance(level, carried)
                wigner[where_to(level - 16), :] = carried[1]
                return carried

            empty = placed[0, 0:DEVICES, :] * 0.0
            carried = lax.fori_loop(0, 16, lower, (empty, empty))
            carried = lax.fori_loop(16, LOW, middle, carried)
            lax.fori_loop(LOW, SPREAD, upper, carried)

    with jax.named_scope("send_late"):

        @pl.when(lax.axis_index("grp") == 1)
        def _():
            send(1)

    smallest = jnp.minimum(2 * me, 2 * DEVICES - 1 - 2 * me)
    first_block = jnp.maximum(smallest // 16 - 1, 0)
    total[...] = jnp.zeros((PACKED * CHANNELS, 128), F32)
    for n in range(2):
        for channel in range(CHANNELS):
            coef_ref[n, channel, :LOW, :] = jnp.zeros((LOW, SPREAD), F32)
    low_lanes = lax.broadcasted_iota(jnp.int32, (8, 128), 1) < 64

    scale = 8.0 * jnp.sqrt(2.0 * degree + 1.0)
    upper_weight = jnp.broadcast_to(order[7:8, :], (16, 128)).astype(BF16)
    lane = lax.broadcasted_iota(jnp.int32, (1, 128), 1)
    lower_weight = jnp.broadcast_to(jnp.where(lane % LOW == 0, 1.0, 2.0), (16, 128)).astype(BF16)
    upper_degrees = 2.0 * (LOW + lane % LOW).astype(F32) + 1.0
    lower_degrees = 2.0 * (lane // 64 * 16 + lane % 16).astype(F32) + 1.0
    upper_inverse = 1.0 / (upper_degrees * upper_degrees)
    lower_inverse = 1.0 / (lower_degrees * lower_degrees)

    def contract(k, begin, end):
        def fold(index, _):
            row = index * 8
            values = received[pl.ds(pl.multiple_of(row, 8), 8), :]
            received[pl.ds(pl.multiple_of(row + 2 * HALF, 8), 8), :] = jnp.where(
                low_lanes, values, pltpu.roll(values, 64, 1)
            )
            return 0

        lax.fori_loop(k * DEVICES + begin, k * DEVICES + end, fold, 0, unroll=8)

        def level_block(block, _):
            shift = jnp.where(block == 0, 2 * HALF, 0)
            rows = [pl.ds(pl.multiple_of(block * 128 + t * 8, 8), 8) for t in range(16)]
            sums = tuple(total[rows[t], :] for t in range(16))

            def gather(group, sums):
                sums = list(sums)
                base = group * 16
                for index in range(16):
                    values = received[
                        pl.ds(
                            pl.multiple_of(shift + base * 8, 8) + (k * DEVICES + begin + index) * 8, 8
                        ),
                        :,
                    ]
                    for t in range(16):
                        factor = wigner[
                            pl.ds(
                                block * 16 * GRID + base + (t * GRID + k * DEVICES + begin + index),
                                8,
                                stride=0,
                            ),
                            :,
                        ]
                        sums[t] = sums[t] + values * factor
                return tuple(sums)

            sums = lax.fori_loop(0, (end - begin) // 16, gather, sums)
            for t in range(16):
                total[rows[t], :] = sums[t]
            return 0

        lax.fori_loop(first_block, 3, level_block, 0)

    for k in range(2):
        for begin, end in CHUNKS[k][::-1]:
            count = min(end, OTHERS) - begin
            with jax.named_scope(f"wait{k}_{begin}"):
                pltpu.make_async_remote_copy(
                    src_ref=spectrum.at[0 : count * 8, :],
                    dst_ref=received.at[0 : count * 8, :],
                    send_sem=send_sem.at[0],
                    recv_sem=recv_sem.at[chunk_of(k, begin)],
                    device_id={"beta": target(OFFSETS[0])},
                    device_id_type=MESH,
                ).wait_recv()
            with jax.named_scope(f"contract{k}_{begin}"):
                contract(k, begin, end)

    with jax.named_scope("finish"):
        lower_scale = jnp.where(
            lax.broadcasted_iota(jnp.int32, (16, 128), 1) < 64, scale[0:16, :], scale[16:32, :]
        )
        lower, upper = [], []
        for channel in range(CHANNELS):
            lower.append(total[pl.ds(channel, 16, stride=CHANNELS), :] * lower_scale)
            upper.append(total[pl.ds(16 * CHANNELS + channel, LOW, stride=CHANNELS), :] * scale[LOW:, :])

        def energies(values):
            squares = [values[f] * values[f] + values[f + 4] * values[f + 4] for f in range(FUNCTIONS)]
            return jnp.concatenate(squares, axis=0)

        def lane_sum(multiplicity, squares):
            return sum(
                lax.dot_general(
                    multiplicity, part, (((1,), (1,)), ((), ())), preferred_element_type=F32
                )
                for part in split(squares)
            )

        first_half = lax.broadcasted_iota(jnp.int32, (64, 128), 1) < 64
        folded = energies(lower)
        folded = jnp.concatenate(
            [jnp.where(first_half, folded, 0.0), jnp.where(first_half, 0.0, folded)], axis=0
        )
        shares[me, 0:1, :] = lane_sum(upper_weight, energies(upper))[0:1] * upper_inverse
        shares[me, 1:2, :] = lane_sum(lower_weight, folded)[0:1] * lower_inverse

    with jax.named_scope("share_send"):
        for offset in OFFSETS:
            pltpu.make_async_remote_copy(
                src_ref=shares.at[me],
                dst_ref=shares.at[me],
                send_sem=send_sem.at[1],
                recv_sem=recv_sem.at[chunk_of(2, 0)],
                device_id={"beta": target(offset)},
                device_id_type=MESH,
            ).start()

    with jax.named_scope("store"):
        for channel in range(CHANNELS):
            for n in range(2):
                begin, end = n * LOW, (n + 1) * LOW
                coef_ref[n, channel, 0:16, :LOW] = lower[channel][:, begin:end]
                coef_ref[n, channel, 16:LOW, :LOW] = lower[channel][:, 64 + begin : 64 + end]
                coef_ref[n, channel, LOW:, :LOW] = upper[channel][:, begin:end]
                coef_ref[n, channel, LOW:, LOW:] = upper[channel][:, 64 + begin : 64 + end]

    with jax.named_scope("sent"):
        for k in range(2):
            pltpu.make_async_remote_copy(
                src_ref=spectrum.at[0 : OTHERS * 8, :],
                dst_ref=received.at[0 : OTHERS * 8, :],
                send_sem=send_sem.at[0],
                recv_sem=recv_sem.at[0],
                device_id={"beta": target(OFFSETS[0])},
                device_id_type=MESH,
            ).wait_send()

    with jax.named_scope("share_wait"):
        shared = pltpu.make_async_remote_copy(
            src_ref=shares.at[0:OTHERS],
            dst_ref=shares.at[0:OTHERS],
            send_sem=send_sem.at[1],
            recv_sem=recv_sem.at[chunk_of(2, 0)],
            device_id={"beta": target(OFFSETS[0])},
            device_id_type=MESH,
        )
        shared.wait_send()
        shared.wait_recv()


def tail(coef_ref, shares, coef_hbm, power_hbm, power, sem):
    store = pltpu.make_async_copy(coef_ref, coef_hbm, sem.at[0])
    store.start()
    sums = [shares[index] for index in range(4)]
    for index in range(4, DEVICES):
        sums[index % 4] = sums[index % 4] + shares[index]
    result = (sums[0] + sums[1]) + (sums[2] + sums[3])
    for f in range(FUNCTIONS):
        power[f : f + 1, 0:16] = result[1:2, f * 16 : f * 16 + 16]
        power[f : f + 1, 16:LOW] = result[1:2, 64 + f * 16 : 64 + f * 16 + 16]
        power[f : f + 1, LOW:] = result[0:1, f * LOW : (f + 1) * LOW]
    finish = pltpu.make_async_copy(power, power_hbm, sem.at[1])
    finish.start()
    store.wait()
    finish.wait()


def local(samples):
    packed, twist = fourier_tables()
    anywhere = pl.BlockSpec(memory_space=pl.ANY)
    vmem = pl.BlockSpec(memory_space=pltpu.VMEM)
    coef, shares = pl.pallas_call(
        body,
        out_shape=(
            pltpu.VMEM((2, CHANNELS, SPREAD, SPREAD), F32),
            pltpu.VMEM((DEVICES, 2, 128), F32),
        ),
        in_specs=[anywhere] * 5,
        out_specs=(vmem, vmem),
        scratch_shapes=[
            pltpu.VMEM((2, FUNCTIONS, GRID, GRID), F32),
            pltpu.VMEM((640, 256), BF16),
            pltpu.VMEM((256, 128), F32),
            pltpu.VMEM((512, 128), F32),
            pltpu.VMEM((8, 128), F32),
            pltpu.VMEM((2 * HALF, 128), F32),
            pltpu.VMEM((4 * HALF, 128), F32),
            pltpu.VMEM((PACKED * GRID, 128), F32),
            pltpu.VMEM((PACKED * CHANNELS, 128), F32),
            pltpu.VMEM((3, SPREAD, 128), F32),
            pltpu.VMEM((2, GRID, 128), F32),
            pltpu.SemaphoreType.DMA((6,)),
            pltpu.SemaphoreType.DMA((2,)),
            pltpu.SemaphoreType.DMA((sum(map(len, CHUNKS)),)),
        ],
        compiler_params=pltpu.CompilerParams(collective_id=0, has_side_effects=True),
        name="rotation_transform",
    )(samples, packed, twist, beta_tables(), order_tables())
    coef, power = pl.pallas_call(
        tail,
        out_shape=(
            jax.ShapeDtypeStruct((2, CHANNELS, SPREAD, SPREAD), F32),
            jax.ShapeDtypeStruct((FUNCTIONS, SPREAD), F32),
        ),
        in_specs=[vmem, vmem],
        out_specs=(anywhere, anywhere),
        scratch_shapes=[pltpu.VMEM((FUNCTIONS, SPREAD), F32), pltpu.SemaphoreType.DMA((2,))],
        compiler_params=pltpu.CompilerParams(vmem_limit_bytes=4 * 1024 * 1024),
        name="store_results",
    )(coef, shares)
    return coef.reshape(2, 2, FUNCTIONS, SPREAD, SPREAD), power


def solution(mesh):
    return jax.shard_map(
        local,
        mesh=mesh,
        in_specs=(P("beta", "grp", None, None),),
        out_specs=(P("beta", None, "grp", None, None), P("grp", None)),
        check_vma=False,
    )
```

```python
import itertools
import math

import jax
import jax.numpy as jnp
import numpy as np
from jax import lax
from jax.experimental import pallas as pl
from jax.experimental.pallas import tpu as pltpu
from jax.sharding import PartitionSpec as P

MESH = pl.DeviceIdType.MESH
F32 = jnp.float32
BF16 = jnp.bfloat16

GRID = 128
SPREAD = 64
FUNCTIONS = 4
CHANNELS = 8
DEVICES = 64
OTHERS = DEVICES - 1
HALF = DEVICES * CHANNELS
SEND_COST = (0.0, 1.0, 2.2, 1.65)
GREET_COST = (0.0, 1.65, 2.2, 1.0)


def far_first(cost):
    near = [o for o in itertools.product(range(4), repeat=3) if o != (0, 0, 0)]
    order = []
    for z, y, x in near:
        for turn in ((z, y, x), (y, x, z), (x, z, y)):
            for offset in (turn, tuple((4 - step) % 4 for step in turn)):
                if offset not in order:
                    order.append(offset)
    return sorted(order, key=lambda o: -sum(cost[step] for step in o))


OFFSETS = far_first(SEND_COST)
GREETINGS = far_first(GREET_COST)
CHUNKS = (((0, 16), (16, 32), (32, 48), (48, 64)), ((0, 16), (16, 32), (32, 48), (48, 64)), ((0, 64),))


def split_bf16(table):
    high = jnp.asarray(table, F32).astype(BF16)
    low = (jnp.asarray(table, F32) - high.astype(F32)).astype(BF16)
    return high, low


def fourier_tables():
    g = np.arange(GRID)
    q = np.arange(SPREAD)
    gamma = 2.0 * np.pi * ((g[:, None] * q[None, :]) % GRID) / GRID
    cosine, minus_sine = np.cos(gamma), -np.sin(gamma)
    first = np.concatenate([cosine, cosine, minus_sine, minus_sine], axis=1)
    j = np.arange(DEVICES)
    alpha = 2.0 * np.pi * ((2 * j[:, None] * g[None, :]) % GRID) / GRID
    c, s = np.cos(alpha) / GRID, np.sin(alpha) / GRID
    second = np.concatenate(
        [np.concatenate([c, s], axis=1), np.concatenate([-s, c], axis=1)], axis=0
    )
    first_high, first_low = split_bf16(first)
    packed = jnp.concatenate([first_high, first_high, first_low, *split_bf16(second)], axis=0)
    turn = 2.0 * np.pi * g / GRID
    ones = np.ones((GRID, SPREAD))
    twist_cos = np.concatenate([ones, np.cos(turn)[:, None] * ones], axis=1)
    twist_sin = np.concatenate([0.0 * ones, np.sin(turn)[:, None] * ones], axis=1)
    return packed, jnp.asarray(np.concatenate([twist_cos, twist_sin], axis=0), F32)


def beta_tables():
    k = np.arange(GRID).reshape(DEVICES, 2).T.reshape(GRID)
    angles = np.pi * (2 * k + 1) / 256.0
    odd = 2.0 * np.arange(SPREAD) + 1.0
    weight = (2.0 / SPREAD) * np.sin(angles)
    weight = weight * np.sum(np.sin(angles[:, None] * odd) / odd, axis=1)
    columns = [np.cos(angles), np.log(np.cos(angles / 2)), np.log(np.sin(angles / 2)), weight]
    tables = [np.repeat(column[:, None], GRID, axis=1) for column in columns]
    return jnp.asarray(np.concatenate(tables, axis=0), F32)


def order_tables():
    lgamma = np.array([math.lgamma(v + 1.0) for v in range(2 * GRID + 1)])
    n = np.arange(GRID)
    p = np.where(n < SPREAD, n, n - GRID)[:, None]
    q = np.arange(SPREAD)[None, :]
    lowest = np.maximum(np.abs(p), q)
    t = np.maximum(0, q - p)
    magnitude = 0.5 * (
        lgamma[lowest + p] + lgamma[lowest - p] + lgamma[lowest + q] + lgamma[lowest - q]
    )
    magnitude = magnitude - lgamma[lowest + q - t] - lgamma[t]
    magnitude = magnitude - lgamma[p - q + t] - lgamma[lowest - p - t]
    sign = 1.0 - 2.0 * ((p - q + t) % 2)
    cos_power = 2 * lowest + q - p - 2 * t
    sin_power = p - q + 2 * t
    multiplicity = np.where(q == 0, 1.0, 2.0)
    rows = [magnitude, sign, cos_power, sin_power, lowest, p, q, multiplicity]
    rows = [np.broadcast_to(row, (GRID, SPREAD)).reshape(DEVICES, 1, 2 * SPREAD) for row in rows]
    return jnp.asarray(np.concatenate(rows, axis=1), F32)


def chunk_of(k, slot):
    before = sum(len(chunks) for chunks in CHUNKS[:k])
    return before + next(i for i, (_, end) in enumerate(CHUNKS[k]) if slot < end)


def tile(index):
    return pl.ds(pl.multiple_of(index * 8, 8), 8)


def body(
    samples_hbm,
    packed_hbm,
    twist_hbm,
    beta_hbm,
    order_hbm,
    coef_ref,
    shares,
    samples,
    packed,
    twist,
    beta,
    order,
    spectrum,
    received,
    wigner,
    total,
    rows_of_level,
    placed,
    load_sem,
    send_sem,
    recv_sem,
):
    me = lax.axis_index("beta")
    place = (me // 16, me // 4 % 4, me % 4)

    def target(offset):
        z, y, x = ((place[axis] + offset[axis]) % 4 for axis in range(3))
        return z * 16 + y * 4 + x

    loads = [
        pltpu.make_async_copy(packed_hbm, packed, load_sem.at[0]),
        pltpu.make_async_copy(samples_hbm.at[0], samples.at[0], load_sem.at[1]),
        pltpu.make_async_copy(twist_hbm, twist, load_sem.at[2]),
        pltpu.make_async_copy(samples_hbm.at[1], samples.at[1], load_sem.at[3]),
        pltpu.make_async_copy(beta_hbm, beta, load_sem.at[4]),
        pltpu.make_async_copy(order_hbm.at[me], order, load_sem.at[5]),
    ]
    for load in loads:
        load.start()

    barrier = pltpu.get_barrier_semaphore()
    with jax.named_scope("greet"):
        for offset in GREETINGS:
            pl.semaphore_signal(
                barrier, 1, device_id={"beta": target(offset)}, device_id_type=MESH
            )

    def product(left, right):
        return jnp.dot(left, right, preferred_element_type=F32)

    def split(values):
        high = values.astype(BF16)
        return high, (values - high.astype(F32)).astype(BF16)

    def transform(k):
        high, low = split(samples[k].reshape(FUNCTIONS * GRID, GRID))
        halfway = product(jnp.concatenate([high, low], axis=1), packed[0:256, :])
        halfway = halfway + product(high, packed[256:384, :])
        twist_cos, twist_sin = twist[0:128, :], twist[128:256, :]
        alpha_high, alpha_low = packed[384:512, :], packed[512:640, :]
        for pair in range(2):
            turned = []
            for f in (2 * pair, 2 * pair + 1):
                part = halfway[f * GRID : (f + 1) * GRID]
                re, im = part[:, :128], part[:, 128:]
                turned.append(
                    jnp.concatenate(
                        [twist_cos * re + twist_sin * im, twist_cos * im - twist_sin * re], axis=0
                    )
                )
            turned_high, turned_low = split(jnp.concatenate(turned, axis=1))
            rows = (
                product(alpha_high, turned_high)
                + product(alpha_low, turned_high)
                + product(alpha_high, turned_low)
            )
            for s in range(2):
                for f in range(2):
                    spectrum[
                        pl.ds(k * HALF + s * FUNCTIONS + 2 * pair + f, DEVICES, stride=8), :
                    ] = rows[s * DEVICES : (s + 1) * DEVICES, f * 128 : (f + 1) * 128]

    def send(k):
        for slot, offset in enumerate(OFFSETS):
            other = target(offset)
            pltpu.make_async_remote_copy(
                src_ref=spectrum.at[tile(k * DEVICES + other), :],
                dst_ref=received.at[pl.ds(k * HALF + slot * 8, 8), :],
                send_sem=send_sem.at[0],
                recv_sem=recv_sem.at[chunk_of(k, slot)],
                device_id={"beta": other},
                device_id_type=MESH,
            ).start()

    with jax.named_scope("load0"):
        for load in loads[:3]:
            load.wait()
    with jax.named_scope("dft0"):
        transform(0)
    with jax.named_scope("load1"):
        for load in loads[3:]:
            load.wait()
    with jax.named_scope("dft1"):
        transform(1)
    with jax.named_scope("barrier_wait"):
        pl.semaphore_wait(barrier, OTHERS)
    with jax.named_scope("send"):
        send(0)

        @pl.when(lax.axis_index("grp") == 0)
        def _():
            send(1)
    for k in range(2):
        received[k * HALF + OTHERS * 8 : (k + 1) * HALF, :] = spectrum[tile(k * DEVICES + me), :]

    with jax.named_scope("coeff"):
        alpha_order, gamma_order = order[5:6, :], order[6:7, :]
        lowest = order[4:5, :]
        degree = lax.broadcasted_iota(jnp.int32, (SPREAD, 128), 0).astype(F32)
        previous = degree - 1.0
        upper = (degree * degree - alpha_order * alpha_order) * (
            degree * degree - gamma_order * gamma_order
        )
        lower = (previous * previous - alpha_order * alpha_order) * (
            previous * previous - gamma_order * gamma_order
        )
        root_upper = jnp.sqrt(jnp.maximum(upper, 1.0))
        rows_of_level[0] = degree * (2.0 * previous + 1.0) / root_upper
        rows_of_level[1] = alpha_order * gamma_order / jnp.maximum(previous * degree, 1.0)
        rows_of_level[2] = (
            degree * jnp.sqrt(jnp.maximum(lower, 0.0)) / (jnp.maximum(previous, 1.0) * root_upper)
        )
        beta[128:256, :] = (
            beta[384:512, :]
            * order[1:2, :]
            * jnp.exp(
                order[0:1, :] + order[2:3, :] * beta[128:256, :] + order[3:4, :] * beta[256:384, :]
            )
        )

    with jax.named_scope("arrange"):
        for slot, offset in enumerate(OFFSETS + [(0, 0, 0)]):
            sender = target(tuple((4 - step) % 4 for step in offset))
            for k in range(2):
                for table in range(2):
                    placed[table, k * DEVICES + slot : k * DEVICES + slot + 1, :] = beta[
                        pl.ds(sender + table * GRID + k * DEVICES, 1), :
                    ]

    with jax.named_scope("wigner"):
        for k in range(2):

            def advance(level, carried):
                former, current = carried
                f_row = rows_of_level[0, pl.ds(level, 1), :]
                c_row = rows_of_level[1, pl.ds(level, 1), :]
                b_row = rows_of_level[2, pl.ds(level, 1), :]
                starts = lowest == level.astype(F32)
                cosine = placed[0, k * DEVICES : (k + 1) * DEVICES, :]
                first = placed[1, k * DEVICES : (k + 1) * DEVICES, :]
                recurred = f_row * (cosine - c_row) * current - b_row * former
                renewed = jnp.where(starts, first, recurred)
                wigner[pl.ds(pl.multiple_of(level * GRID + k * DEVICES, 64), DEVICES), :] = renewed
                return current, renewed

            empty = placed[0, 0:DEVICES, :] * 0.0
            lax.fori_loop(0, SPREAD, advance, (empty, empty))

    with jax.named_scope("send_late"):

        @pl.when(lax.axis_index("grp") == 1)
        def _():
            send(1)

    smallest = jnp.minimum(2 * me, 2 * DEVICES - 1 - 2 * me)
    first_block = smallest // 32
    total[...] = jnp.zeros(total.shape, F32)

    def contract(k, begin, end):
        def level_block(block, _):
            rows = [pl.ds(pl.multiple_of(block * 256 + t * 8, 8), 8) for t in range(32)]
            sums = tuple(total[rows[t], :] for t in range(32))

            def gather(group, sums):
                sums = list(sums)
                base = group * 16
                for index in range(16):
                    values = received[
                        pl.ds(pl.multiple_of(base * 8, 8) + (k * DEVICES + begin + index) * 8, 8), :
                    ]
                    for t in range(32):
                        factor = wigner[
                            pl.ds(
                                block * 32 * GRID + base + (t * GRID + k * DEVICES + begin + index),
                                8,
                                stride=0,
                            ),
                            :,
                        ]
                        sums[t] = sums[t] + values * factor
                return tuple(sums)

            sums = lax.fori_loop(0, (end - begin) // 16, gather, sums)
            for t in range(32):
                total[rows[t], :] = sums[t]
            return 0

        lax.fori_loop(first_block, 2, level_block, 0)

    for k in range(2):
        for begin, end in CHUNKS[k][::-1]:
            count = min(end, OTHERS) - begin
            with jax.named_scope(f"wait{k}_{begin}"):
                pltpu.make_async_remote_copy(
                    src_ref=spectrum.at[0 : count * 8, :],
                    dst_ref=received.at[0 : count * 8, :],
                    send_sem=send_sem.at[0],
                    recv_sem=recv_sem.at[chunk_of(k, begin)],
                    device_id={"beta": target(OFFSETS[0])},
                    device_id_type=MESH,
                ).wait_recv()
            with jax.named_scope(f"contract{k}_{begin}"):
                contract(k, begin, end)

    with jax.named_scope("finish"):
        scale = 8.0 * jnp.sqrt(2.0 * degree + 1.0)
        coeffs = []
        for channel in range(CHANNELS):
            coeffs.append(total[pl.ds(channel, SPREAD, stride=CHANNELS), :] * scale)
        squares = jnp.concatenate(
            [coeffs[f] * coeffs[f] + coeffs[f + 4] * coeffs[f + 4] for f in range(FUNCTIONS)], axis=0
        )
        squares_high, squares_low = split(squares)
        multiplicity = jnp.broadcast_to(order[7:8, :], (16, 128)).astype(BF16)

        def lane_sum(values):
            return lax.dot_general(
                multiplicity, values, (((1,), (1,)), ((), ())), preferred_element_type=F32
            )

        energy = lane_sum(squares_high) + lane_sum(squares_low)
        lane = lax.broadcasted_iota(jnp.int32, (1, 128), 1)
        degrees = 2.0 * (lane % SPREAD).astype(F32) + 1.0
        inverse = 1.0 / (degrees * degrees)
        shares[me, 0:1, :] = energy[0:1, :128] * inverse
        shares[me, 1:2, :] = energy[0:1, 128:] * inverse

    with jax.named_scope("share_send"):
        for offset in OFFSETS:
            pltpu.make_async_remote_copy(
                src_ref=shares.at[me],
                dst_ref=shares.at[me],
                send_sem=send_sem.at[1],
                recv_sem=recv_sem.at[chunk_of(2, 0)],
                device_id={"beta": target(offset)},
                device_id_type=MESH,
            ).start()

    with jax.named_scope("store"):
        for channel in range(CHANNELS):
            coef_ref[0, channel] = coeffs[channel][:, :SPREAD]
            coef_ref[1, channel] = coeffs[channel][:, SPREAD:]

    with jax.named_scope("sent"):
        for k in range(2):
            pltpu.make_async_remote_copy(
                src_ref=spectrum.at[0 : OTHERS * 8, :],
                dst_ref=received.at[0 : OTHERS * 8, :],
                send_sem=send_sem.at[0],
                recv_sem=recv_sem.at[0],
                device_id={"beta": target(OFFSETS[0])},
                device_id_type=MESH,
            ).wait_send()

    with jax.named_scope("share_wait"):
        shared = pltpu.make_async_remote_copy(
            src_ref=shares.at[0:OTHERS],
            dst_ref=shares.at[0:OTHERS],
            send_sem=send_sem.at[1],
            recv_sem=recv_sem.at[chunk_of(2, 0)],
            device_id={"beta": target(OFFSETS[0])},
            device_id_type=MESH,
        )
        shared.wait_send()
        shared.wait_recv()


def tail(coef_ref, shares, coef_hbm, power_hbm, power, sem):
    store = pltpu.make_async_copy(coef_ref, coef_hbm, sem.at[0])
    store.start()
    sums = [shares[index] for index in range(4)]
    for index in range(4, DEVICES):
        sums[index % 4] = sums[index % 4] + shares[index]
    result = (sums[0] + sums[1]) + (sums[2] + sums[3])
    for f in range(FUNCTIONS):
        power[f : f + 1, :] = result[f // 2 : f // 2 + 1, f % 2 * 64 : f % 2 * 64 + 64]
    finish = pltpu.make_async_copy(power, power_hbm, sem.at[1])
    finish.start()
    store.wait()
    finish.wait()


def local(samples):
    packed, twist = fourier_tables()
    anywhere = pl.BlockSpec(memory_space=pl.ANY)
    vmem = pl.BlockSpec(memory_space=pltpu.VMEM)
    coef, shares = pl.pallas_call(
        body,
        out_shape=(
            pltpu.VMEM((2, CHANNELS, SPREAD, SPREAD), F32),
            pltpu.VMEM((DEVICES, 2, 128), F32),
        ),
        in_specs=[anywhere] * 5,
        out_specs=(vmem, vmem),
        scratch_shapes=[
            pltpu.VMEM((2, FUNCTIONS, GRID, GRID), F32),
            pltpu.VMEM((640, 256), BF16),
            pltpu.VMEM((256, 128), F32),
            pltpu.VMEM((512, 128), F32),
            pltpu.VMEM((8, 128), F32),
            pltpu.VMEM((2 * HALF + 8, 128), F32),
            pltpu.VMEM((2 * HALF, 128), F32),
            pltpu.VMEM((SPREAD * GRID + 8, 128), F32),
            pltpu.VMEM((SPREAD * CHANNELS + 8, 128), F32),
            pltpu.VMEM((3, SPREAD, 128), F32),
            pltpu.VMEM((2, GRID, 128), F32),
            pltpu.SemaphoreType.DMA((6,)),
            pltpu.SemaphoreType.DMA((2,)),
            pltpu.SemaphoreType.DMA((sum(map(len, CHUNKS)),)),
        ],
        compiler_params=pltpu.CompilerParams(collective_id=0, has_side_effects=True),
        name="rotation_transform",
    )(samples, packed, twist, beta_tables(), order_tables())
    coef, power = pl.pallas_call(
        tail,
        out_shape=(
            jax.ShapeDtypeStruct((2, CHANNELS, SPREAD, SPREAD), F32),
            jax.ShapeDtypeStruct((FUNCTIONS, SPREAD), F32),
        ),
        in_specs=[vmem, vmem],
        out_specs=(anywhere, anywhere),
        scratch_shapes=[pltpu.VMEM((FUNCTIONS, SPREAD), F32), pltpu.SemaphoreType.DMA((2,))],
        compiler_params=pltpu.CompilerParams(vmem_limit_bytes=4 * 1024 * 1024),
        name="store_results",
    )(coef, shares)
    return coef.reshape(2, 2, FUNCTIONS, SPREAD, SPREAD), power


def solution(mesh):
    return jax.shard_map(
        local,
        mesh=mesh,
        in_specs=(P("beta", "grp", None, None),),
        out_specs=(P("beta", None, "grp", None, None), P("grp", None)),
        check_vma=False,
    )
```

```python
import itertools
import math

import jax
import jax.numpy as jnp
import numpy as np
from jax import lax
from jax.experimental import pallas as pl
from jax.experimental.pallas import tpu as pltpu
from jax.sharding import PartitionSpec as P

MESH = pl.DeviceIdType.MESH
F32 = jnp.float32
BF16 = jnp.bfloat16

GRID = 128
SPREAD = 64
FUNCTIONS = 4
CHANNELS = 8
DEVICES = 64
OTHERS = DEVICES - 1
HALF = DEVICES * CHANNELS
SEND_COST = (0.0, 1.0, 2.2, 1.65)
GREET_COST = (0.0, 1.65, 2.2, 1.0)


def far_first(cost):
    near = [o for o in itertools.product(range(4), repeat=3) if o != (0, 0, 0)]
    order = []
    for z, y, x in near:
        for turn in ((z, y, x), (y, x, z), (x, z, y)):
            for offset in (turn, tuple((4 - step) % 4 for step in turn)):
                if offset not in order:
                    order.append(offset)
    return sorted(order, key=lambda o: -sum(cost[step] for step in o))


OFFSETS = far_first(SEND_COST)
GREETINGS = far_first(GREET_COST)
CHUNKS = (((0, 16), (16, 32), (32, 48), (48, 64)), ((0, 16), (16, 32), (32, 48), (48, 64)), ((0, 64),))


def split_bf16(table):
    high = jnp.asarray(table, F32).astype(BF16)
    low = (jnp.asarray(table, F32) - high.astype(F32)).astype(BF16)
    return high, low


def fourier_tables():
    g = np.arange(GRID)
    q = np.arange(SPREAD)
    gamma = 2.0 * np.pi * ((g[:, None] * q[None, :]) % GRID) / GRID
    cosine, minus_sine = np.cos(gamma), -np.sin(gamma)
    first = np.concatenate([cosine, cosine, minus_sine, minus_sine], axis=1)
    j = np.arange(DEVICES)
    alpha = 2.0 * np.pi * ((2 * j[:, None] * g[None, :]) % GRID) / GRID
    c, s = np.cos(alpha) / GRID, np.sin(alpha) / GRID
    second = np.concatenate(
        [np.concatenate([c, s], axis=1), np.concatenate([-s, c], axis=1)], axis=0
    )
    first_high, first_low = split_bf16(first)
    packed = jnp.concatenate([first_high, first_high, first_low, *split_bf16(second)], axis=0)
    turn = 2.0 * np.pi * g / GRID
    ones = np.ones((GRID, SPREAD))
    twist_cos = np.concatenate([ones, np.cos(turn)[:, None] * ones], axis=1)
    twist_sin = np.concatenate([0.0 * ones, np.sin(turn)[:, None] * ones], axis=1)
    return packed, jnp.asarray(np.concatenate([twist_cos, twist_sin], axis=0), F32)


def beta_tables():
    k = np.arange(GRID).reshape(DEVICES, 2).T.reshape(GRID)
    angles = np.pi * (2 * k + 1) / 256.0
    odd = 2.0 * np.arange(SPREAD) + 1.0
    weight = (2.0 / SPREAD) * np.sin(angles)
    weight = weight * np.sum(np.sin(angles[:, None] * odd) / odd, axis=1)
    columns = [np.cos(angles), np.log(np.cos(angles / 2)), np.log(np.sin(angles / 2)), weight]
    tables = [np.repeat(column[:, None], GRID, axis=1) for column in columns]
    return jnp.asarray(np.concatenate(tables, axis=0), F32)


def order_tables():
    lgamma = np.array([math.lgamma(v + 1.0) for v in range(2 * GRID + 1)])
    n = np.arange(GRID)
    p = np.where(n < SPREAD, n, n - GRID)[:, None]
    q = np.arange(SPREAD)[None, :]
    lowest = np.maximum(np.abs(p), q)
    t = np.maximum(0, q - p)
    magnitude = 0.5 * (
        lgamma[lowest + p] + lgamma[lowest - p] + lgamma[lowest + q] + lgamma[lowest - q]
    )
    magnitude = magnitude - lgamma[lowest + q - t] - lgamma[t]
    magnitude = magnitude - lgamma[p - q + t] - lgamma[lowest - p - t]
    sign = 1.0 - 2.0 * ((p - q + t) % 2)
    cos_power = 2 * lowest + q - p - 2 * t
    sin_power = p - q + 2 * t
    multiplicity = np.where(q == 0, 1.0, 2.0)
    rows = [magnitude, sign, cos_power, sin_power, lowest, p, q, multiplicity]
    rows = [np.broadcast_to(row, (GRID, SPREAD)).reshape(DEVICES, 1, 2 * SPREAD) for row in rows]
    return jnp.asarray(np.concatenate(rows, axis=1), F32)


def chunk_of(k, slot):
    before = sum(len(chunks) for chunks in CHUNKS[:k])
    return before + next(i for i, (_, end) in enumerate(CHUNKS[k]) if slot < end)


def tile(index):
    return pl.ds(pl.multiple_of(index * 8, 8), 8)


def body(
    samples_hbm,
    packed_hbm,
    twist_hbm,
    beta_hbm,
    order_hbm,
    coef_ref,
    shares,
    samples,
    packed,
    twist,
    beta,
    order,
    spectrum,
    received,
    wigner,
    total,
    rows_of_level,
    placed,
    load_sem,
    send_sem,
    recv_sem,
):
    me = lax.axis_index("beta")
    place = (me // 16, me // 4 % 4, me % 4)

    def target(offset):
        z, y, x = ((place[axis] + offset[axis]) % 4 for axis in range(3))
        return z * 16 + y * 4 + x

    loads = [
        pltpu.make_async_copy(packed_hbm, packed, load_sem.at[0]),
        pltpu.make_async_copy(samples_hbm.at[0], samples.at[0], load_sem.at[1]),
        pltpu.make_async_copy(twist_hbm, twist, load_sem.at[2]),
        pltpu.make_async_copy(samples_hbm.at[1], samples.at[1], load_sem.at[3]),
        pltpu.make_async_copy(beta_hbm, beta, load_sem.at[4]),
        pltpu.make_async_copy(order_hbm.at[me], order, load_sem.at[5]),
    ]
    barrier = pltpu.get_barrier_semaphore()

    def greet(offsets):
        for offset in offsets:
            pl.semaphore_signal(
                barrier, 1, device_id={"beta": target(offset)}, device_id_type=MESH
            )

    with jax.named_scope("greet"):
        greet(GREETINGS[:7])
        for load in loads:
            load.start()
        greet(GREETINGS[7:])

    def product(left, right):
        return jnp.dot(left, right, preferred_element_type=F32)

    def split(values):
        high = values.astype(BF16)
        return high, (values - high.astype(F32)).astype(BF16)

    def transform(k):
        high, low = split(samples[k].reshape(FUNCTIONS * GRID, GRID))
        halfway = product(jnp.concatenate([high, low], axis=1), packed[0:256, :])
        halfway = halfway + product(high, packed[256:384, :])
        twist_cos, twist_sin = twist[0:128, :], twist[128:256, :]
        alpha_high, alpha_low = packed[384:512, :], packed[512:640, :]
        for pair in range(2):
            turned = []
            for f in (2 * pair, 2 * pair + 1):
                part = halfway[f * GRID : (f + 1) * GRID]
                re, im = part[:, :128], part[:, 128:]
                turned.append(
                    jnp.concatenate(
                        [twist_cos * re + twist_sin * im, twist_cos * im - twist_sin * re], axis=0
                    )
                )
            turned_high, turned_low = split(jnp.concatenate(turned, axis=1))
            rows = (
                product(alpha_high, turned_high)
                + product(alpha_low, turned_high)
                + product(alpha_high, turned_low)
            )
            for s in range(2):
                for f in range(2):
                    spectrum[
                        pl.ds(k * HALF + s * FUNCTIONS + 2 * pair + f, DEVICES, stride=8), :
                    ] = rows[s * DEVICES : (s + 1) * DEVICES, f * 128 : (f + 1) * 128]

    def send(k):
        for slot, offset in enumerate(OFFSETS):
            other = target(offset)
            pltpu.make_async_remote_copy(
                src_ref=spectrum.at[tile(k * DEVICES + other), :],
                dst_ref=received.at[pl.ds(k * HALF + slot * 8, 8), :],
                send_sem=send_sem.at[0],
                recv_sem=recv_sem.at[chunk_of(k, slot)],
                device_id={"beta": other},
                device_id_type=MESH,
            ).start()

    with jax.named_scope("load0"):
        for load in loads[:3]:
            load.wait()
    with jax.named_scope("dft0"):
        transform(0)
    with jax.named_scope("load1"):
        for load in loads[3:]:
            load.wait()
    with jax.named_scope("dft1"):
        transform(1)
    with jax.named_scope("barrier_wait"):
        pl.semaphore_wait(barrier, OTHERS)
    with jax.named_scope("send"):
        send(0)

        @pl.when(lax.axis_index("grp") == 0)
        def _():
            send(1)
    for k in range(2):
        received[k * HALF + OTHERS * 8 : (k + 1) * HALF, :] = spectrum[tile(k * DEVICES + me), :]

    with jax.named_scope("coeff"):
        alpha_order, gamma_order = order[5:6, :], order[6:7, :]
        lowest = order[4:5, :]
        degree = lax.broadcasted_iota(jnp.int32, (SPREAD, 128), 0).astype(F32)
        previous = degree - 1.0
        upper = (degree * degree - alpha_order * alpha_order) * (
            degree * degree - gamma_order * gamma_order
        )
        lower = (previous * previous - alpha_order * alpha_order) * (
            previous * previous - gamma_order * gamma_order
        )
        root_upper = jnp.sqrt(jnp.maximum(upper, 1.0))
        rows_of_level[0] = degree * (2.0 * previous + 1.0) / root_upper
        rows_of_level[1] = alpha_order * gamma_order / jnp.maximum(previous * degree, 1.0)
        rows_of_level[2] = (
            degree * jnp.sqrt(jnp.maximum(lower, 0.0)) / (jnp.maximum(previous, 1.0) * root_upper)
        )
        beta[128:256, :] = (
            beta[384:512, :]
            * order[1:2, :]
            * jnp.exp(
                order[0:1, :] + order[2:3, :] * beta[128:256, :] + order[3:4, :] * beta[256:384, :]
            )
        )

    with jax.named_scope("arrange"):
        for slot, offset in enumerate(OFFSETS + [(0, 0, 0)]):
            sender = target(tuple((4 - step) % 4 for step in offset))
            for k in range(2):
                for table in range(2):
                    placed[table, k * DEVICES + slot : k * DEVICES + slot + 1, :] = beta[
                        pl.ds(sender + table * GRID + k * DEVICES, 1), :
                    ]

    with jax.named_scope("wigner"):
        for k in range(2):

            def advance(level, carried):
                former, current = carried
                f_row = rows_of_level[0, pl.ds(level, 1), :]
                c_row = rows_of_level[1, pl.ds(level, 1), :]
                b_row = rows_of_level[2, pl.ds(level, 1), :]
                starts = lowest == level.astype(F32)
                cosine = placed[0, k * DEVICES : (k + 1) * DEVICES, :]
                first = placed[1, k * DEVICES : (k + 1) * DEVICES, :]
                recurred = f_row * (cosine - c_row) * current - b_row * former
                renewed = jnp.where(starts, first, recurred)
                wigner[pl.ds(pl.multiple_of(level * GRID + k * DEVICES, 64), DEVICES), :] = renewed
                return current, renewed

            empty = placed[0, 0:DEVICES, :] * 0.0
            lax.fori_loop(0, SPREAD, advance, (empty, empty))

    with jax.named_scope("send_late"):

        @pl.when(lax.axis_index("grp") == 1)
        def _():
            send(1)

    smallest = jnp.minimum(2 * me, 2 * DEVICES - 1 - 2 * me)
    first_block = smallest // 32
    total[...] = jnp.zeros(total.shape, F32)

    def contract(k, begin, end):
        def level_block(block, _):
            rows = [pl.ds(pl.multiple_of(block * 256 + t * 8, 8), 8) for t in range(32)]
            sums = tuple(total[rows[t], :] for t in range(32))

            def gather(group, sums):
                sums = list(sums)
                base = group * 16
                for index in range(16):
                    values = received[
                        pl.ds(pl.multiple_of(base * 8, 8) + (k * DEVICES + begin + index) * 8, 8), :
                    ]
                    for t in range(32):
                        factor = wigner[
                            pl.ds(
                                block * 32 * GRID + base + (t * GRID + k * DEVICES + begin + index),
                                8,
                                stride=0,
                            ),
                            :,
                        ]
                        sums[t] = sums[t] + values * factor
                return tuple(sums)

            sums = lax.fori_loop(0, (end - begin) // 16, gather, sums)
            for t in range(32):
                total[rows[t], :] = sums[t]
            return 0

        lax.fori_loop(first_block, 2, level_block, 0)

    for k in range(2):
        for begin, end in CHUNKS[k][::-1]:
            count = min(end, OTHERS) - begin
            with jax.named_scope(f"wait{k}_{begin}"):
                pltpu.make_async_remote_copy(
                    src_ref=spectrum.at[0 : count * 8, :],
                    dst_ref=received.at[0 : count * 8, :],
                    send_sem=send_sem.at[0],
                    recv_sem=recv_sem.at[chunk_of(k, begin)],
                    device_id={"beta": target(OFFSETS[0])},
                    device_id_type=MESH,
                ).wait_recv()
            with jax.named_scope(f"contract{k}_{begin}"):
                contract(k, begin, end)

    with jax.named_scope("finish"):
        scale = 8.0 * jnp.sqrt(2.0 * degree + 1.0)
        coeffs = []
        for channel in range(CHANNELS):
            coeffs.append(total[pl.ds(channel, SPREAD, stride=CHANNELS), :] * scale)
        squares = jnp.concatenate(
            [coeffs[f] * coeffs[f] + coeffs[f + 4] * coeffs[f + 4] for f in range(FUNCTIONS)], axis=0
        )
        multiplicity = jnp.broadcast_to(order[7:8, :], (16, 128)).astype(BF16)
        energy = lax.dot_general(
            jnp.concatenate([multiplicity, multiplicity], axis=1),
            jnp.concatenate(split(squares), axis=1),
            (((1,), (1,)), ((), ())),
            preferred_element_type=F32,
        )
        lane = lax.broadcasted_iota(jnp.int32, (1, 128), 1)
        degrees = 2.0 * (lane % SPREAD).astype(F32) + 1.0
        inverse = 1.0 / (degrees * degrees)
        shares[me, 0:1, :] = energy[0:1, :128] * inverse
        shares[me, 1:2, :] = energy[0:1, 128:] * inverse

    with jax.named_scope("share_send"):
        for offset in OFFSETS:
            pltpu.make_async_remote_copy(
                src_ref=shares.at[me],
                dst_ref=shares.at[me],
                send_sem=send_sem.at[1],
                recv_sem=recv_sem.at[chunk_of(2, 0)],
                device_id={"beta": target(offset)},
                device_id_type=MESH,
            ).start()

    with jax.named_scope("store"):
        for channel in range(CHANNELS):
            coef_ref[0, channel] = coeffs[channel][:, :SPREAD]
            coef_ref[1, channel] = coeffs[channel][:, SPREAD:]

    with jax.named_scope("sent"):
        for k in range(2):
            pltpu.make_async_remote_copy(
                src_ref=spectrum.at[0 : OTHERS * 8, :],
                dst_ref=received.at[0 : OTHERS * 8, :],
                send_sem=send_sem.at[0],
                recv_sem=recv_sem.at[0],
                device_id={"beta": target(OFFSETS[0])},
                device_id_type=MESH,
            ).wait_send()

    with jax.named_scope("share_wait"):
        shared = pltpu.make_async_remote_copy(
            src_ref=shares.at[0:OTHERS],
            dst_ref=shares.at[0:OTHERS],
            send_sem=send_sem.at[1],
            recv_sem=recv_sem.at[chunk_of(2, 0)],
            device_id={"beta": target(OFFSETS[0])},
            device_id_type=MESH,
        )
        shared.wait_send()
        shared.wait_recv()


def tail(coef_ref, shares, coef_hbm, power_hbm, power, sem):
    store = pltpu.make_async_copy(coef_ref, coef_hbm, sem.at[0])
    store.start()
    sums = [shares[index] for index in range(4)]
    for index in range(4, DEVICES):
        sums[index % 4] = sums[index % 4] + shares[index]
    result = (sums[0] + sums[1]) + (sums[2] + sums[3])
    for f in range(FUNCTIONS):
        power[f : f + 1, :] = result[f // 2 : f // 2 + 1, f % 2 * 64 : f % 2 * 64 + 64]
    finish = pltpu.make_async_copy(power, power_hbm, sem.at[1])
    finish.start()
    store.wait()
    finish.wait()


def local(samples):
    packed, twist = fourier_tables()
    anywhere = pl.BlockSpec(memory_space=pl.ANY)
    vmem = pl.BlockSpec(memory_space=pltpu.VMEM)
    coef, shares = pl.pallas_call(
        body,
        out_shape=(
            pltpu.VMEM((2, CHANNELS, SPREAD, SPREAD), F32),
            pltpu.VMEM((DEVICES, 2, 128), F32),
        ),
        in_specs=[anywhere] * 5,
        out_specs=(vmem, vmem),
        scratch_shapes=[
            pltpu.VMEM((2, FUNCTIONS, GRID, GRID), F32),
            pltpu.VMEM((640, 256), BF16),
            pltpu.VMEM((256, 128), F32),
            pltpu.VMEM((512, 128), F32),
            pltpu.VMEM((8, 128), F32),
            pltpu.VMEM((2 * HALF + 8, 128), F32),
            pltpu.VMEM((2 * HALF, 128), F32),
            pltpu.VMEM((SPREAD * GRID + 8, 128), F32),
            pltpu.VMEM((SPREAD * CHANNELS + 8, 128), F32),
            pltpu.VMEM((3, SPREAD, 128), F32),
            pltpu.VMEM((2, GRID, 128), F32),
            pltpu.SemaphoreType.DMA((6,)),
            pltpu.SemaphoreType.DMA((2,)),
            pltpu.SemaphoreType.DMA((sum(map(len, CHUNKS)),)),
        ],
        compiler_params=pltpu.CompilerParams(collective_id=0, has_side_effects=True),
        name="rotation_transform",
    )(samples, packed, twist, beta_tables(), order_tables())
    coef, power = pl.pallas_call(
        tail,
        out_shape=(
            jax.ShapeDtypeStruct((2, CHANNELS, SPREAD, SPREAD), F32),
            jax.ShapeDtypeStruct((FUNCTIONS, SPREAD), F32),
        ),
        in_specs=[vmem, vmem],
        out_specs=(anywhere, anywhere),
        scratch_shapes=[pltpu.VMEM((FUNCTIONS, SPREAD), F32), pltpu.SemaphoreType.DMA((2,))],
        compiler_params=pltpu.CompilerParams(vmem_limit_bytes=4 * 1024 * 1024),
        name="store_results",
    )(coef, shares)
    return coef.reshape(2, 2, FUNCTIONS, SPREAD, SPREAD), power


def solution(mesh):
    return jax.shard_map(
        local,
        mesh=mesh,
        in_specs=(P("beta", "grp", None, None),),
        out_specs=(P("beta", None, "grp", None, None), P("grp", None)),
        check_vma=False,
    )
```
